32 devices in a mesh: band: 4 (over y, x), slab: 8 (over z, core).
Axes of the slice: x: 2, y: 2, z: 4, core: 2. Of those that a mesh axis runs over, the one named last changes fastest.
Arguments:
- band_block: float32 [4, 2, 2, 128, 128, 128], P(None, None, None, 'band', 'slab'), may hold values from -24 to 24
- material_grid: int32 [128, 128, 128], P('slab'), may hold values from 0 to 3
- inverse_permittivity: float32 [4], replicated, may hold values from 0.077 to 1
- bloch_index: int32 [1], replicated, may hold values from 0 to 7
Outputs:
- search_block: float32 [4, 2, 2, 128, 128, 128], P(None, None, None, 'band', 'slab')
- correlation: float32 [2, 8, 8], replicated
- projected: float32 [2, 8, 8], replicated
The draws below stay inside these ranges and needn't reach their ends.
All inputs are finite; a program needn't handle non-finite values.
Results may differ from the reference program's by a relative error of at most 0.00005.
Values sent between devices are 32-bit elements; how exact they have to be, the bound alone decides.
A program may use at most 192 MiB of HBM per device.

```python
import math
import jax
import jax.numpy as jnp
from jax import lax

NX = 128
NY = 128
NZ = 128
MATERIALS = 4
KPOINTS = 8
BANDS = 4
NPTS = 2097152


def signed_fraction(length):
    indices = jnp.arange(length, dtype=jnp.int32)
    signed = jnp.where(indices >= length // 2, indices - length, indices).astype(jnp.float32)
    return signed / length


def draw_band_block(key, part):
    own_key = jax.random.fold_in(key, 11)
    common_key = jax.random.fold_in(key, 12)
    grid_shape = (BANDS, 2, 2, NZ, NY, NX)
    common = jnp.clip(jax.random.normal(common_key, (1, 2, 2, NZ, NY, NX), jnp.float32), -4.0, 4.0)
    own = jnp.clip(jax.random.normal(own_key, grid_shape, jnp.float32), -4.0, 4.0)
    depth_part = signed_fraction(NZ)[:, None, None]
    height_part = signed_fraction(NY)[None, :, None]
    width_part = signed_fraction(NX)[None, None, :]
    envelope = 3.0 / (1.0 + 12.0 * (depth_part * depth_part + height_part * height_part + width_part * width_part))
    return (envelope * (own + 0.7 * common)).astype(jnp.float32)


def set_ends(drawn, key, smallest, largest):
    index_at = [jax.random.randint(jax.random.fold_in(key, axis), (), 0, length) for axis, length in enumerate(drawn.shape)]
    longest = drawn.shape.index(max(drawn.shape))
    next_to = index_at[:longest] + [(index_at[longest] + 1) % drawn.shape[longest]] + index_at[longest + 1:]
    return drawn.at[tuple(index_at)].set(smallest).at[tuple(next_to)].set(largest)


def setup_inputs(seed: int = 0) -> dict:
    key_list = jax.random.split(jax.random.key(seed), 5)
    band_block = draw_band_block(jax.random.fold_in(key_list[4], 71), 0)
    material_grid = set_ends(jax.random.randint(key_list[1], (NZ, NY, NX), 0, MATERIALS), jax.random.fold_in(key_list[1], 1), 0, MATERIALS - 1).astype(jnp.int32)
    inverse_permittivity = jnp.clip(jnp.exp(jax.random.uniform(key_list[2], (MATERIALS,), jnp.float32, math.log(0.077), math.log(1.0))), 0.077, 1.0)
    bloch_index = jax.random.randint(key_list[3], (1,), 0, KPOINTS).astype(jnp.int32)
    return dict(band_block=band_block, material_grid=material_grid, inverse_permittivity=inverse_permittivity, bloch_index=bloch_index)


HIGHEST = lax.Precision.HIGHEST

def axis_values(length, weight, fraction, offset, extent):
    indices = offset + jnp.arange(extent, dtype=jnp.int32)
    signed = jnp.where(indices >= length // 2, indices - length, indices).astype(jnp.float32)
    return 2.0 * math.pi / length * (signed + weight * fraction)

def frame(depth_wave, height_wave, width_wave):
    depth_term = depth_wave[:, None, None]
    height_term = height_wave[None, :, None]
    width_term = width_wave[None, None, :]
    planar = jnp.sqrt(width_term * width_term + height_term * height_term)
    magnitude = jnp.sqrt(planar * planar + depth_term * depth_term)
    grid_shape = magnitude.shape
    primary = [jnp.broadcast_to(height_term / planar, grid_shape), jnp.broadcast_to(-width_term / planar, grid_shape), jnp.zeros(grid_shape, magnitude.dtype)]
    secondary = [width_term * depth_term / (magnitude * planar), height_term * depth_term / (magnitude * planar), jnp.broadcast_to(-planar / magnitude, grid_shape)]
    return (primary, secondary, magnitude)

def curl_field(block, primary, secondary, magnitude):
    first_comp = block[:, 0]
    second_comp = block[:, 1]
    parts = [magnitude * (first_comp * secondary[component] - second_comp * primary[component]) for component in range(3)]
    return jnp.stack(parts, axis=1).reshape((-1,) + first_comp.shape[1:])

def project_back(spectrum, primary, secondary, magnitude, band_count):
    grouped = spectrum.reshape((band_count, 3) + spectrum.shape[1:])
    along_second = grouped[:, 0] * secondary[0] + grouped[:, 1] * secondary[1] + grouped[:, 2] * secondary[2]
    along_primary = grouped[:, 0] * primary[0] + grouped[:, 1] * primary[1] + grouped[:, 2] * primary[2]
    return jnp.stack([magnitude * along_second, -magnitude * along_primary], axis=1)

def operate(block, inverse_cells, primary, secondary, magnitude):

    def one_band(single):
        curled = curl_field(single[None], primary, secondary, magnitude)
        spectrum = curled[:, 0] + 1j * curled[:, 1]
        spatial = jnp.fft.ifftn(spectrum, axes=(1, 2, 3)) * inverse_cells
        returned = jnp.fft.fftn(spatial, axes=(1, 2, 3))
        values = jnp.stack([jnp.real(returned), jnp.imag(returned)], axis=1)
        return project_back(values, primary, secondary, magnitude, 1)[0]
    return lax.map(one_band, block)

def gram_parts(left, right):
    left_real = left[:, :, 0].reshape(left.shape[0], -1)
    left_imag = left[:, :, 1].reshape(left.shape[0], -1)
    right_real = right[:, :, 0].reshape(right.shape[0], -1)
    right_imag = right[:, :, 1].reshape(right.shape[0], -1)
    inner_product = lambda first_rows, second_rows: jnp.einsum('km,jm->kj', first_rows, second_rows, precision=HIGHEST)
    real_sum = inner_product(left_real, right_real) + inner_product(left_imag, right_imag)
    imag_sum = inner_product(left_real, right_imag) - inner_product(left_imag, right_real)
    return (real_sum / NPTS, imag_sum / NPTS)

def reference(band_block, material_grid, inverse_permittivity, bloch_index):
    fraction = (bloch_index[0].astype(jnp.float32) + 1.0) / KPOINTS
    primary, secondary, magnitude = frame(axis_values(NZ, 0.2, fraction, 0, NZ), axis_values(NY, 0.35, fraction, 0, NY), axis_values(NX, 0.5, fraction, 0, NX))
    inverse_cells = inverse_permittivity[material_grid]
    image = operate(band_block, inverse_cells, primary, secondary, magnitude)
    correlation_real, correlation_imag = gram_parts(band_block, band_block)
    cross_real, cross_imag = gram_parts(band_block, image)
    system = jnp.concatenate([jnp.concatenate([correlation_real, -correlation_imag], 1), jnp.concatenate([correlation_imag, correlation_real], 1)], 0)
    right_side = jnp.concatenate([cross_real, cross_imag], 0)
    solution = jnp.linalg.solve(system, right_side)
    mixing_real = solution[:BANDS]
    mixing_imag = solution[BANDS:]
    block_real = band_block[:, :, 0]
    block_imag = band_block[:, :, 1]
    combine = lambda data, mixing: jnp.einsum('iabcd,ij->jabcd', data, mixing, precision=HIGHEST)
    residual_real = image[:, :, 0] - (combine(block_real, mixing_real) - combine(block_imag, mixing_imag))
    residual_imag = image[:, :, 1] - (combine(block_real, mixing_imag) + combine(block_imag, mixing_real))
    search_block = jnp.stack([residual_real, residual_imag], axis=2) / (magnitude * magnitude + 1.0)
    search_image = operate(search_block, inverse_cells, primary, secondary, magnitude)
    stacked = jnp.concatenate([band_block, search_block], 0)
    images = jnp.concatenate([image, search_image], 0)
    full_real, full_imag = gram_parts(stacked, stacked)
    proj_real, proj_imag = gram_parts(stacked, images)
    return (search_block, jnp.stack([full_real, full_imag], 0), jnp.stack([proj_real, proj_imag], 0))
```

```python
from functools import partial
import math

import jax
import jax.numpy as jnp
import numpy as np
from jax import lax
from jax.experimental import pallas as pl
from jax.experimental.pallas import tpu as pltpu
from jax.sharding import PartitionSpec as P

KPOINTS = 8
HIGHEST = lax.Precision.HIGHEST
MESH = pl.DeviceIdType.MESH
VMEM_LIMIT = 60 * 1024 * 1024


def axis_values(length, weight, fraction, offset, extent):
    indices = offset + jnp.arange(extent, dtype=jnp.int32)
    signed = jnp.where(indices >= length // 2, indices - length, indices).astype(jnp.float32)
    return 2.0 * math.pi / length * (signed + weight * fraction)


def halves(values):
    high = values.astype(jnp.bfloat16)
    return high, (values - high.astype(jnp.float32)).astype(jnp.bfloat16)


def dft_matrix(length, direction):
    indices = np.arange(length)
    angles = 2.0 * np.pi / length * (np.outer(indices, indices) % length)
    cosine, sine = np.cos(angles), direction * np.sin(angles)
    return np.block([[cosine, -sine], [sine, cosine]])


def numpy_halves(matrix):
    single = matrix.astype(np.float32)
    high = single.astype(jnp.bfloat16)
    low = (single - high.astype(np.float32)).astype(jnp.bfloat16)
    return high, low


def left_table(length, direction):
    return np.concatenate(numpy_halves(dft_matrix(length, direction)), 0)


def right_table(matrix):
    high, low = numpy_halves(matrix)
    return np.concatenate([high, high, low], 0)


def dot(left, right):
    return jnp.dot(left, right, preferred_element_type=jnp.float32)


def left_transform(table, values):
    size = values.shape[0]
    high, low = halves(values)
    main = dot(table[...], high)
    rest = dot(table[:size, :], low)
    return main[:size] + (main[size:] + rest)


def right_transform(values, table):
    high, low = halves(values)
    return dot(jnp.concatenate([high, low, high], 1), table[...])


def step_count(size):
    return 2 if size % 2 == 0 else 1


def gram(acc, base, hermitian, left, right, count, depth_of):
    bands, rows, lanes = left.shape[0], left.shape[4], left.shape[5]
    for i in range(bands):
        others = list(range(i if hermitian else 0, bands))

        def body(step, sums, i=i, others=others):
            depth = depth_of(step)
            sums = list(sums)
            for row in range(0, rows, 8):
                tile = (depth, pl.ds(row, 8), slice(None))
                for comp in range(2):
                    left_real = left[(i, comp, 0) + tile]
                    left_imag = left[(i, comp, 1) + tile]
                    for place, j in enumerate(others):
                        right_real = right[(j, comp, 0) + tile]
                        right_imag = right[(j, comp, 1) + tile]
                        sums[2 * place] += left_real * right_real + left_imag * right_imag
                        sums[2 * place + 1] += left_real * right_imag - left_imag * right_real
            return tuple(sums)

        zeros = tuple(jnp.zeros((8, lanes), jnp.float32) for _ in range(2 * len(others)))
        sums = lax.fori_loop(0, count, body, zeros)
        for place, value in enumerate(sums):
            acc[base + place] += value
        base += 2 * len(others)
    return base


def gram_rows(bands, hermitian):
    return bands * (bands + 1) if hermitian else 2 * bands * bands


def unpack(flat, bands, hermitian):
    real = [[None] * bands for _ in range(bands)]
    imag = [[None] * bands for _ in range(bands)]
    place = 0
    for i in range(bands):
        for j in range(i if hermitian else 0, bands):
            real[i][j], imag[i][j] = flat[place], flat[place + 1]
            if hermitian and j > i:
                real[j][i], imag[j][i] = flat[place], -flat[place + 1]
            place += 2
    stack = lambda rows: jnp.stack([jnp.stack(row) for row in rows])
    return stack(real), stack(imag)


class Place:
    def __init__(self, groups, slabs):
        self.groups, self.slabs = groups, slabs
        self.group = lax.axis_index("band")
        self.slab = lax.axis_index("slab")
        self.layer, self.core = self.slab // 2, self.slab % 2
        self.cell = 2 * self.group + self.core

    def slab_peer(self, step):
        slab = lax.rem(self.slab + step, self.slabs)
        return slab, (self.group, slab)

    def band_peer(self, step):
        group = lax.rem(self.group + step, self.groups)
        return group, (group, self.slab)

    def plane_peer(self, step):
        cell = lax.rem(self.cell + step, 2 * self.groups)
        return cell, (cell // 2, 2 * self.layer + cell % 2)


def enter(devices):
    barrier = pltpu.get_barrier_semaphore()
    for device in devices:
        pl.semaphore_signal(barrier, inc=1, device_id=device, device_id_type=MESH)
    pl.semaphore_wait(barrier, len(devices))


def send(source, target, send_sem, recv_sem, device):
    pltpu.make_async_remote_copy(
        src_ref=source,
        dst_ref=target,
        send_sem=send_sem,
        recv_sem=recv_sem,
        device_id=device,
        device_id_type=MESH,
    ).start()


def await_bytes(ref, sem):
    pltpu.make_async_copy(ref, ref, sem).wait()


def total(place, mine, first, second, sems, values):
    mine[0] = values
    first[place.slab] = values
    for step in range(1, place.slabs):
        _, device = place.slab_peer(step)
        send(mine.at[0], first.at[place.slab], sems.at[0], sems.at[1], device)
    await_bytes(first.at[pl.ds(0, place.slabs - 1)], sems.at[1])
    values = first[0]
    for slab in range(1, place.slabs):
        values = values + first[slab]
    mine[1] = values
    second[place.group] = values
    for step in range(1, place.groups):
        _, device = place.band_peer(step)
        send(mine.at[1], second.at[place.group], sems.at[2], sems.at[3], device)
    await_bytes(second.at[pl.ds(0, place.groups - 1)], sems.at[3])
    values = second[0]
    for group in range(1, place.groups):
        values = values + second[group]
    await_bytes(first.at[pl.ds(0, place.slabs - 1)], sems.at[0])
    await_bytes(second.at[pl.ds(0, place.groups - 1)], sems.at[2])
    return values


def lane_sums(tile, acc):
    rows = acc.shape[0]
    tile[...] = jnp.zeros_like(tile)
    tile[:rows, :] = jnp.sum(acc[...], axis=1)
    ones = jnp.ones((8, tile.shape[1]), jnp.float32)
    return lax.dot_general(
        ones, tile[...], (((1,), (1,)), ((), ())), precision=HIGHEST,
        preferred_element_type=jnp.float32,
    )


def first_kernel(
    groups, slabs, block, waves, depths, cells, x_plus, y_plus, z_plus, z_minus, y_minus, x_minus,
    image, sums, work, out_y, in_z, out_z, in_y, eta, acc, tile, mine, first, second, sems, tail,
):
    place = Place(groups, slabs)
    bands, _, _, depth, rows, width = block.shape
    half = depth // 2
    height = rows * slabs
    length = depth * groups
    share = out_y.shape[3] // half
    step = step_count(half)
    chunks = half // step
    part = step * share

    enter(
        [place.slab_peer(i)[1] for i in range(1, slabs)]
        + [
            (lax.rem(place.group + i, groups), 2 * place.layer + core)
            for i in range(1, groups)
            for core in range(2)
        ]
    )

    @pl.loop(0, chunks)
    def _(k):
        for i in range(1, slabs):
            slab, device = place.slab_peer(i)
            send(
                block.at[slab // 2, :, :, pl.ds(half * (slab % 2) + k * step, step), :, :],
                work.at[:, :, pl.ds(k * step, step), pl.ds(rows * place.slab, rows), :],
                sems.at[0, k], sems.at[1, k], device,
            )

    slab_cells = cells.shape[1]
    for i in range(1, slabs):
        slab, device = place.slab_peer(i)
        send(
            cells.at[2 * place.group + slab % 2],
            eta.at[pl.ds(slab_cells * place.slab, slab_cells), :],
            tail.at[4], tail.at[5], device,
        )
    eta[pl.ds(slab_cells * place.slab, slab_cells), :] = cells[place.cell]

    acc[...] = jnp.zeros_like(acc)
    gram(acc, 0, True, block, block, depth, lambda t: t)

    @pl.loop(0, chunks)
    def _(k):
        await_bytes(
            work.at[:, :, pl.ds(0, step), pl.ds(0, rows * (slabs - 1)), :], sems.at[1, k]
        )

        @pl.loop(0, step)
        def _(i):
            z = k * step + i
            for comp in range(2):
                for ri in range(2):
                    work[comp, ri, z, pl.ds(rows * place.slab, rows), :] = block[
                        place.layer, comp, ri, half * place.core + z
                    ]
            across, along, planar = waves[0], waves[1], waves[2]
            deep = depths[half * place.core + z, 0:1, :]
            size = jnp.sqrt(planar * planar + deep * deep)
            fields = []
            for ri in range(2):
                one = work[0, ri, z]
                two = work[1, ri, z] * size
                upright = one * deep
                fields.append(
                    [across * upright - along * two, along * upright + across * two, -planar * one]
                )
            curled = jnp.concatenate(
                [jnp.concatenate([fields[0][c], fields[1][c]], 1) for c in range(3)], 0
            )
            lines = right_transform(curled, x_plus)
            stacked = jnp.concatenate(
                [
                    jnp.concatenate(
                        [
                            lines[c * height : (c + 1) * height, :width],
                            lines[c * height : (c + 1) * height, width:],
                        ],
                        0,
                    )
                    for c in range(3)
                ],
                1,
            )
            planes = left_transform(y_plus, stacked)
            for c in range(3):
                for ri in range(2):
                    for cell in range(2 * groups):
                        base = ri * height + cell * share
                        out_y[cell, c, ri, pl.ds(z * share, share), :] = planes[
                            base : base + share, c * width : (c + 1) * width
                        ]

        for i in range(1, 2 * groups):
            cell, device = place.plane_peer(i)
            send(
                out_y.at[cell, :, :, pl.ds(k * part, part), :],
                in_z.at[:, :, pl.ds(place.cell * half * share + k * part, part), :],
                sems.at[2, k], sems.at[3, k], device,
            )
        for c in range(3):
            for ri in range(2):
                in_z[c, ri, pl.ds(place.cell * half * share + k * part, part), :] = out_y[
                    place.cell, c, ri, pl.ds(k * part, part), :
                ]

    await_bytes(eta.at[pl.ds(0, slab_cells * (slabs - 1)), :], tail.at[5])

    @pl.loop(0, chunks)
    def _(k):
        await_bytes(in_z.at[:, :, pl.ds(0, part * (2 * groups - 1)), :], sems.at[3, k])

    @pl.loop(0, share // 2)
    def _(pair):
        weights = [eta[pl.ds(2 * pair + j, length, stride=share), :] for j in range(2)]
        for c in range(3):
            stacked = jnp.concatenate(
                [
                    jnp.concatenate(
                        [in_z[c, ri, pl.ds(2 * pair + j, length, stride=share), :] for ri in range(2)],
                        0,
                    )
                    for j in range(2)
                ],
                1,
            )
            field = left_transform(z_plus, stacked)
            weight = jnp.concatenate(weights, 1)
            field = field * jnp.concatenate([weight, weight], 0)
            back = left_transform(z_minus, field)
            for j in range(2):
                for ri in range(2):
                    out_z[c, ri, pl.ds(2 * pair + j, length, stride=share), :] = back[
                        ri * length : (ri + 1) * length, j * width : (j + 1) * width
                    ]

    @pl.loop(0, chunks)
    def _(k):
        for i in range(1, 2 * groups):
            cell, device = place.plane_peer(i)
            send(
                out_z.at[:, :, pl.ds(cell * half * share + k * part, part), :],
                in_y.at[place.cell, :, :, pl.ds(k * part, part), :],
                sems.at[4, k], sems.at[5, k], device,
            )

    @pl.loop(0, chunks)
    def _(k):
        for c in range(3):
            for ri in range(2):
                in_y[place.cell, c, ri, pl.ds(k * part, part), :] = out_z[
                    c, ri, pl.ds(place.cell * half * share + k * part, part), :
                ]
        await_bytes(
            in_y.at[pl.ds(0, 2 * groups - 1), :, :, pl.ds(0, part), :], sems.at[5, k]
        )

        @pl.loop(0, step)
        def _(i):
            z = k * step + i
            stacked = jnp.concatenate(
                [
                    jnp.concatenate(
                        [
                            in_y[cell, c, ri, pl.ds(z * share, share), :]
                            for ri in range(2)
                            for cell in range(2 * groups)
                        ],
                        0,
                    )
                    for c in range(3)
                ],
                1,
            )
            planes = left_transform(y_minus, stacked)
            lines = jnp.concatenate(
                [
                    jnp.concatenate(
                        [
                            planes[:height, c * width : (c + 1) * width],
                            planes[height:, c * width : (c + 1) * width],
                        ],
                        1,
                    )
                    for c in range(3)
                ],
                0,
            )
            curled = right_transform(lines, x_minus)
            across, along, planar = waves[0], waves[1], waves[2]
            deep = depths[half * place.core + z, 0:1, :]
            size = jnp.sqrt(planar * planar + deep * deep)
            for ri in range(2):
                fields = [
                    curled[c * height : (c + 1) * height, ri * width : (ri + 1) * width]
                    for c in range(3)
                ]
                work[0, ri, z] = deep * (across * fields[0] + along * fields[1]) - planar * fields[2]
                work[1, ri, z] = size * (across * fields[1] - along * fields[0])
            for comp in range(2):
                for ri in range(2):
                    image[place.layer, comp, ri, half * place.core + z] = work[
                        comp, ri, z, pl.ds(rows * place.slab, rows), :
                    ]

        for i in range(1, slabs):
            slab, device = place.slab_peer(i)
            send(
                work.at[:, :, pl.ds(k * step, step), pl.ds(rows * slab, rows), :],
                image.at[place.layer, :, :, pl.ds(half * place.core + k * step, step), :, :],
                sems.at[6, k], sems.at[7, k], device,
            )

    @pl.loop(0, chunks)
    def _(k):
        await_bytes(
            work.at[:, :, pl.ds(0, step), pl.ds(0, rows * (slabs - 1)), :], sems.at[7, k]
        )
        gram(
            acc, gram_rows(bands, True), True, block, image, 2 * step,
            lambda t: half * (t // step) + k * step + t % step,
        )

    sums[...] = total(place, mine, first, second, tail, lane_sums(tile, acc))

    @pl.loop(0, chunks)
    def _(k):
        slab_bytes = work.at[:, :, pl.ds(0, step), pl.ds(0, rows * (slabs - 1)), :]
        plane_bytes = in_z.at[:, :, pl.ds(0, part * (2 * groups - 1)), :]
        await_bytes(slab_bytes, sems.at[0, k])
        await_bytes(plane_bytes, sems.at[2, k])
        await_bytes(plane_bytes, sems.at[4, k])
        await_bytes(slab_bytes, sems.at[6, k])

    await_bytes(eta.at[pl.ds(0, slab_cells * (slabs - 1)), :], tail.at[4])


def second_kernel(
    groups, slabs, mixing, block, image, waves, depths, cells, x_plus, z_plus, y_plus,
    search, sums, out_x, in_z, out_z, in_y, eta, acc, field_acc, tile, mine, first, second,
    sems, tail,
):
    place = Place(groups, slabs)
    bands, _, _, depth, rows, width = block.shape
    length = depth * groups
    height = rows * slabs
    parts = rows // 8
    thin = length // slabs
    quarter = width // groups
    share = cells.shape[1] // thin

    enter(
        [place.slab_peer(i)[1] for i in range(1, slabs)]
        + [place.band_peer(i)[1] for i in range(1, groups)]
    )
    acc[...] = jnp.zeros_like(acc)
    field_acc[...] = jnp.zeros_like(field_acc)
    lane = lax.broadcasted_iota(jnp.int32, (1, width), 1) // quarter
    deep_step = 8 if depth % 8 == 0 else 1

    @pl.loop(0, parts)
    def _(part):
        band_rows = pl.ds(part * 8, 8)
        across, along, planar = (waves[place.slab, i, band_rows, :] for i in range(3))

        @pl.loop(0, depth)
        def _(z):
            tile_at = (z, band_rows, slice(None))
            deep = depths[z]
            scale = 1.0 / (planar * planar + deep * deep + 1.0)
            for comp in range(2):
                reals = [block[(i, comp, 0) + tile_at] for i in range(bands)]
                imags = [block[(i, comp, 1) + tile_at] for i in range(bands)]
                for j in range(bands):
                    real = image[(j, comp, 0) + tile_at]
                    imag = image[(j, comp, 1) + tile_at]
                    for i in range(bands):
                        real = real - (reals[i] * mixing[i, j] - imags[i] * mixing[bands + i, j])
                        imag = imag - (reals[i] * mixing[bands + i, j] + imags[i] * mixing[i, j])
                    search[(j, comp, 0) + tile_at] = real * scale
                    search[(j, comp, 1) + tile_at] = imag * scale

        @pl.loop(0, depth // deep_step)
        def _(group):
            planes = pl.ds(group * deep_step, deep_step)
            deep = depths[planes]
            size = jnp.sqrt(planar * planar + deep * deep)
            count = deep_step * 8
            lines = []
            for i in range(bands):
                fields = []
                for ri in range(2):
                    one = search[i, 0, ri, planes, band_rows, :]
                    two = search[i, 1, ri, planes, band_rows, :] * size
                    upright = one * deep
                    fields.append(
                        [
                            value.reshape(count, width)
                            for value in (
                                across * upright - along * two,
                                along * upright + across * two,
                                -planar * one,
                            )
                        ]
                    )
                curled = jnp.concatenate(
                    [jnp.concatenate([fields[0][c], fields[1][c]], 1) for c in range(3)], 0
                )
                lines.append(right_transform(curled, x_plus.at[i]))
            at = pl.ds(group * count, count)
            for target in range(groups):
                for ri in range(2):
                    columns = slice(ri * width, (ri + 1) * width)
                    packed = lines[(-target) % groups][:, columns]
                    for spot in range(1, groups):
                        packed = jnp.where(
                            lane == spot, lines[(spot - target) % groups][:, columns], packed
                        )
                    for c in range(3):
                        out_x[part, target, c, ri, at, :] = packed[c * count : (c + 1) * count]

        for c in range(3):
            for i in range(1, groups):
                group, device = place.band_peer(i)
                send(
                    out_x.at[part, group, c],
                    in_z.at[part, c, :, pl.ds(depth * 8 * place.group, depth * 8), :],
                    sems.at[0, part * 3 + c], sems.at[1, part * 3 + c], device,
                )
            for ri in range(2):
                in_z[part, c, ri, pl.ds(depth * 8 * place.group, depth * 8), :] = out_x[
                    part, place.group, c, ri
                ]

    @pl.loop(0, 3 * parts)
    def _(k):
        part, c = k // 3, k % 3
        await_bytes(in_z.at[part, c, :, pl.ds(0, depth * 8 * (groups - 1)), :], sems.at[1, k])

        @pl.loop(0, 4)
        def _(pair):
            stacked = jnp.concatenate(
                [
                    jnp.concatenate(
                        [
                            in_z[part, c, ri, pl.ds(2 * pair + j, length, stride=8), :]
                            for ri in range(2)
                        ],
                        0,
                    )
                    for j in range(2)
                ],
                1,
            )
            columns = left_transform(z_plus, stacked)
            for j in range(2):
                for ri in range(2):
                    out_z[part, c, ri, pl.ds(2 * pair + j, length, stride=8), :] = columns[
                        ri * length : (ri + 1) * length, j * width : (j + 1) * width
                    ]

        for i in range(1, slabs):
            slab, device = place.slab_peer(i)
            send(
                out_z.at[part, c, :, pl.ds(thin * 8 * slab, thin * 8), :],
                in_y.at[c, place.slab, part],
                sems.at[2, k], sems.at[3, k], device,
            )
        for ri in range(2):
            in_y[c, place.slab, part, ri] = out_z[
                part, c, ri, pl.ds(thin * 8 * place.slab, thin * 8), :
            ]

    @pl.loop(0, thin)
    def _(z):
        for cell in range(2 * groups):
            values = cells[cell, pl.ds(z * share, share), :]
            values = pltpu.roll(values, lax.rem(width - quarter * place.group, width), 1)
            values = jnp.where(lane == 0, values, 0.0)
            reach = quarter
            while reach < width:
                values = values + pltpu.roll(values, reach, 1)
                reach *= 2
            eta[z, cell * share : (cell + 1) * share, :] = values

    base = gram(acc, 0, False, block, search, depth, lambda t: t)
    base = gram(acc, base, True, search, search, depth, lambda t: t)
    gram(acc, base, False, search, image, depth, lambda t: t)

    for c in range(3):
        for part in range(parts):
            await_bytes(
                in_y.at[c, pl.ds(0, slabs - 1), part], sems.at[3, part * 3 + c]
            )

        @pl.loop(0, thin)
        def _(z, c=c):
            stacked = jnp.concatenate(
                [
                    in_y[c, slab, part, ri, pl.ds(8 * z, 8), :]
                    for ri in range(2)
                    for slab in range(slabs)
                    for part in range(parts)
                ],
                0,
            )
            field = left_transform(y_plus, stacked)
            real, imag = field[:height], field[height:]
            weight = eta[z]
            real_weighted, imag_weighted = real * weight, imag * weight
            for shift in range(bands // 2 + 1):
                if shift == 0:
                    real_other, imag_other = real, imag
                else:
                    real_other = pltpu.roll(real, quarter * shift, 1)
                    imag_other = pltpu.roll(imag, quarter * shift, 1)
                real_term = real_weighted * real_other + imag_weighted * imag_other
                imag_term = real_weighted * imag_other - imag_weighted * real_other
                for place_of, term in ((2 * shift, real_term), (2 * shift + 1, imag_term)):
                    field_acc[place_of] += jnp.sum(term.reshape(height // 8, 8, width), axis=0)

    pieces = jnp.sum(field_acc[...], axis=1)
    pieces = pltpu.roll(pieces, lax.rem(width - quarter * place.group, width), 1)
    values = lane_sums(tile, acc)
    message = jnp.concatenate([values, jnp.zeros((pieces.shape[0], values.shape[1]), jnp.float32)], 0)
    if values.shape[1] > width:
        pieces = jnp.concatenate(
            [pieces, jnp.zeros((pieces.shape[0], values.shape[1] - width), jnp.float32)], 1
        )
    message = jnp.concatenate([values, pieces], 0)
    sums[...] = total(place, mine, first, second, tail, message)

    @pl.loop(0, 3 * parts)
    def _(k):
        await_bytes(in_z.at[0, 0, :, pl.ds(0, depth * 8 * (groups - 1)), :], sems.at[0, k])
        await_bytes(in_y.at[0, pl.ds(0, slabs - 1), 0], sems.at[2, k])


def vmem(count):
    return [pl.BlockSpec(memory_space=pltpu.VMEM)] * count


def round_up(value, step):
    return -(-value // step) * step


def first_operator(block, waves, depths, cells, groups, slabs):
    bands, _, _, depth, rows, width = block.shape
    half, height, length = depth // 2, rows * slabs, depth * groups
    share = height // (2 * groups)
    count = 2 * gram_rows(bands, True)
    lanes = round_up(count, width)
    chunks = half // step_count(half)
    single = lambda *shape: pltpu.VMEM(shape, jnp.float32)
    tables = [
        jnp.asarray(right_table(dft_matrix(width, 1.0).T)),
        jnp.asarray(left_table(height, 1.0)),
        jnp.asarray(left_table(length, 1.0)),
        jnp.asarray(left_table(length, -1.0)),
        jnp.asarray(left_table(height, -1.0)),
        jnp.asarray(right_table(dft_matrix(width, -1.0).T)),
    ]
    return pl.pallas_call(
        partial(first_kernel, groups, slabs),
        in_specs=vmem(4 + len(tables)),
        out_specs=vmem(2),
        out_shape=[
            jax.ShapeDtypeStruct(block.shape, jnp.float32),
            jax.ShapeDtypeStruct((8, lanes), jnp.float32),
        ],
        scratch_shapes=[
            single(2, 2, half, height, width),
            single(2 * groups, 3, 2, half * share, width),
            single(3, 2, length * share, width),
            single(3, 2, length * share, width),
            single(2 * groups, 3, 2, half * share, width),
            single(length * share, width),
            single(count, 8, width),
            single(lanes, width),
            single(2, 8, lanes),
            single(slabs, 8, lanes),
            single(groups, 8, lanes),
            pltpu.SemaphoreType.DMA((8, chunks)),
            pltpu.SemaphoreType.DMA((6,)),
        ],
        compiler_params=pltpu.CompilerParams(
            collective_id=0, has_side_effects=True, vmem_limit_bytes=VMEM_LIMIT
        ),
    )(block, waves, depths, cells, *tables)


def second_operator(mixing, block, image, waves, depths, cells, groups, slabs):
    bands, _, _, depth, rows, width = block.shape
    height, length = rows * slabs, depth * groups
    thin, parts, quarter = length // slabs, rows // 8, width // groups
    count = 2 * gram_rows(bands, False) + gram_rows(bands, True)
    lanes = round_up(count, width)
    field_rows = round_up(2 * (bands // 2 + 1), 8)
    message = (8 + field_rows, lanes)
    single = lambda *shape: pltpu.VMEM(shape, jnp.float32)
    plain = dft_matrix(width, 1.0).T
    orders = []
    for band in range(bands):
        spots = np.arange(width) // quarter
        source = ((spots - band) % groups) * quarter + np.arange(width) % quarter
        orders.append(right_table(plain[:, np.concatenate([source, width + source])]))
    tables = [
        jnp.asarray(np.stack(orders)),
        jnp.asarray(left_table(length, 1.0)),
        jnp.asarray(left_table(height, 1.0)),
    ]
    return pl.pallas_call(
        partial(second_kernel, groups, slabs),
        in_specs=[pl.BlockSpec(memory_space=pltpu.SMEM)] + vmem(5 + len(tables)),
        out_specs=vmem(2),
        out_shape=[
            jax.ShapeDtypeStruct(block.shape, jnp.float32),
            jax.ShapeDtypeStruct(message, jnp.float32),
        ],
        scratch_shapes=[
            single(parts, groups, 3, 2, depth * 8, width),
            single(parts, 3, 2, length * 8, width),
            single(parts, 3, 2, length * 8, width),
            single(3, slabs, parts, 2, thin * 8, width),
            single(thin, height, width),
            single(count, 8, width),
            single(field_rows, 8, width),
            single(lanes, width),
            single(2, *message),
            single(slabs, *message),
            single(groups, *message),
            pltpu.SemaphoreType.DMA((4, 3 * parts)),
            pltpu.SemaphoreType.DMA((4,)),
        ],
        compiler_params=pltpu.CompilerParams(
            collective_id=1, has_side_effects=True, vmem_limit_bytes=VMEM_LIMIT
        ),
    )(mixing, block, image, waves, depths, cells, *tables)


def shards(band_block, material_grid, inverse_permittivity, bloch_index):
    groups, slabs = lax.axis_size("band"), lax.axis_size("slab")
    bands, _, _, depth, rows, width = band_block.shape
    length, height = depth * groups, rows * slabs
    grid_cells = length * height * width
    thin = length // slabs
    share = height // (2 * groups)
    fraction = (bloch_index[0].astype(jnp.float32) + 1.0) / KPOINTS
    width_wave = axis_values(width, 0.5, fraction, 0, width)[None, :]
    height_wave = axis_values(height, 0.35, fraction, 0, height)[:, None]
    planar = jnp.sqrt(width_wave * width_wave + height_wave * height_wave)
    waves = jnp.stack([width_wave / planar, height_wave / planar, planar])
    depth_wave = axis_values(length, 0.2, fraction, lax.axis_index("band") * depth, depth)
    depths = jnp.broadcast_to(depth_wave[:, None, None], (depth, 8, width))
    grouped = material_grid.reshape(thin, 2 * groups, share, width).transpose(1, 0, 2, 3)
    grouped = grouped.reshape(2 * groups, thin * share, width)
    cells = jnp.zeros(grouped.shape, jnp.float32)
    for material in range(inverse_permittivity.shape[0]):
        cells = jnp.where(grouped == material, inverse_permittivity[material] / grid_cells, cells)

    image, sums = first_operator(band_block, waves, depths, cells, groups, slabs)
    size = gram_rows(bands, True)
    flat = sums[0] / grid_cells
    own_real, own_imag = unpack(flat[:size], bands, True)
    cross_real, cross_imag = unpack(flat[size : 2 * size], bands, True)
    join = lambda rows: jnp.concatenate([jnp.concatenate(row, 1) for row in rows], 0)
    system = join([[own_real, -own_imag], [own_imag, own_real]])
    right_side = jnp.concatenate([cross_real, cross_imag], 0)
    factor = jnp.linalg.cholesky(system)
    mixing = jax.scipy.linalg.cho_solve((factor, True), right_side)

    by_slab = waves.reshape(3, slabs, rows, width).transpose(1, 0, 2, 3)
    search_block, sums = second_operator(
        mixing, band_block, image, by_slab, depths, cells, groups, slabs
    )
    sums = sums / grid_cells
    size = 2 * bands * bands
    flat = sums[0]
    mixed_real, mixed_imag = unpack(flat[:size], bands, False)
    search_real, search_imag = unpack(flat[size : size + gram_rows(bands, True)], bands, True)
    flat = flat[size + gram_rows(bands, True) :]
    back_real, back_imag = unpack(flat[:size], bands, False)
    field = sums[8:, :width].reshape(-1, groups, width // groups).sum(2)
    real = [[None] * bands for _ in range(bands)]
    imag = [[None] * bands for _ in range(bands)]
    for i in range(bands):
        for shift in range(bands // 2 + 1):
            j = (i - shift) % bands
            real[i][j], imag[i][j] = field[2 * shift, i], field[2 * shift + 1, i]
            real[j][i], imag[j][i] = real[i][j], -imag[i][j]
    stack = lambda rows: jnp.stack([jnp.stack(row) for row in rows])
    field_real, field_imag = stack(real), stack(imag)
    correlation = jnp.stack(
        [
            join([[own_real, mixed_real], [mixed_real.T, search_real]]),
            join([[own_imag, mixed_imag], [-mixed_imag.T, search_imag]]),
        ]
    )
    projected = jnp.stack(
        [
            join([[cross_real, back_real.T], [back_real, field_real]]),
            join([[cross_imag, -back_imag.T], [back_imag, field_imag]]),
        ]
    )
    return (search_block, correlation, projected)


def solution(mesh):
    return jax.shard_map(
        shards,
        mesh=mesh,
        in_specs=(P(None, None, None, "band", "slab", None), P("slab", None, None), P(), P()),
        out_specs=(P(None, None, None, "band", "slab", None), P(), P()),
        check_vma=False,
    )
```

```python
from functools import partial
import math

import jax
import jax.numpy as jnp
import numpy as np
from jax import lax
from jax.experimental import pallas as pl
from jax.experimental.pallas import tpu as pltpu
from jax.sharding import PartitionSpec as P

KPOINTS = 8
HIGHEST = lax.Precision.HIGHEST
MESH = pl.DeviceIdType.MESH
VMEM_LIMIT = 60 * 1024 * 1024


def halves(values):
    high = values.astype(jnp.bfloat16)
    return high, (values - high.astype(jnp.float32)).astype(jnp.bfloat16)


def dft_matrix(length, direction):
    indices = np.arange(length)
    angles = 2.0 * np.pi / length * (np.outer(indices, indices) % length)
    cosine, sine = np.cos(angles), direction * np.sin(angles)
    return np.block([[cosine, -sine], [sine, cosine]])


def numpy_halves(matrix):
    single = matrix.astype(np.float32)
    high = single.astype(jnp.bfloat16)
    low = (single - high.astype(np.float32)).astype(jnp.bfloat16)
    return high, low


def left_table(length, direction):
    return np.concatenate(numpy_halves(dft_matrix(length, direction)), 0)


def right_table(matrix):
    high, low = numpy_halves(matrix)
    return np.concatenate([high, high, low], 0)


def dot(left, right):
    return jnp.dot(left, right, preferred_element_type=jnp.float32)


def left_transform(table, values):
    size = values.shape[0]
    high, low = halves(values)
    main = dot(table[...], high)
    rest = dot(table[:size, :], low)
    return main[:size] + (main[size:] + rest)


def right_transform(values, table):
    high, low = halves(values)
    return dot(jnp.concatenate([high, low, high], 1), table[...])


def step_count(size):
    return 2 if size % 2 == 0 else 1


def gram(acc, base, hermitian, left, right, count, depth_of):
    bands, rows, lanes = left.shape[0], left.shape[4], left.shape[5]
    for i in range(bands):
        others = list(range(i if hermitian else 0, bands))

        def body(step, sums, i=i, others=others):
            depth = depth_of(step)
            sums = list(sums)
            for row in range(0, rows, 8):
                tile = (depth, pl.ds(row, 8), slice(None))
                for comp in range(2):
                    left_real = left[(i, comp, 0) + tile]
                    left_imag = left[(i, comp, 1) + tile]
                    for place, j in enumerate(others):
                        right_real = right[(j, comp, 0) + tile]
                        right_imag = right[(j, comp, 1) + tile]
                        sums[2 * place] += left_real * right_real + left_imag * right_imag
                        sums[2 * place + 1] += left_real * right_imag - left_imag * right_real
            return tuple(sums)

        zeros = tuple(jnp.zeros((8, lanes), jnp.float32) for _ in range(2 * len(others)))
        sums = lax.fori_loop(0, count, body, zeros)
        for place, value in enumerate(sums):
            acc[base + place] += value
        base += 2 * len(others)
    return base


def gram_rows(bands, hermitian):
    return bands * (bands + 1) if hermitian else 2 * bands * bands


def scatter_tables(entries, pieces, width):
    slots = {}
    rows = 8 * (-(-(1 + max(entry[2] for entry in entries)) // 8))
    for source, lane, row, column, sign in entries:
        columns = slots.setdefault((source, lane), {})
        columns.setdefault(column, {})[row] = sign
    blocks = []
    for source in range(pieces):
        depth = max([len(v) for (s, _), v in slots.items() if s == source], default=0)
        blocks += [(source, place) for place in range(depth)]
    spread = np.zeros((rows, width * len(blocks)), np.float32)
    gather = np.zeros((width * len(blocks), width), np.float32)
    for index, (source, place) in enumerate(blocks):
        for lane in range(width):
            columns = list(slots.get((source, lane), {}).items())
            if place < len(columns):
                column, signs = columns[place]
                gather[index * width + lane, column] = 1.0
                for row, sign in signs.items():
                    spread[row, index * width + lane] = sign
    return [source for source, _ in blocks], spread, gather.astype(jnp.bfloat16)


def scatter(values, sources, spread, gather):
    rows, width = spread.shape[0], values[0].shape[1]
    spots = jnp.concatenate(
        [
            jnp.broadcast_to(values[source], (rows, width))
            * spread[:, place * width : (place + 1) * width]
            for place, source in enumerate(sources)
        ],
        1,
    )
    high, rest = halves(spots)
    low = (spots - high.astype(jnp.float32)) - rest.astype(jnp.float32)
    return (dot(high, gather[...]) + dot(rest, gather[...])) + dot(
        low.astype(jnp.bfloat16), gather[...]
    )


def pair_list(bands, hermitian):
    return [(i, j) for i in range(bands) for j in range(i if hermitian else 0, bands)]


def complex_entries(source, base, pairs, put):
    entries = []
    for place, (i, j) in enumerate(pairs):
        for real_row, imag_row, column, sign in put(i, j):
            lane = base + 2 * place
            entries.append((source + lane // 128, lane % 128, real_row, column, 1.0))
            entries.append((source + (lane + 1) // 128, (lane + 1) % 128, imag_row, column, sign))
    return entries


def mirrored(i, j, put):
    return [put(i, j, 1.0)] if i == j else [put(i, j, 1.0), put(j, i, -1.0)]


def system_entries(bands):
    pairs = pair_list(bands, True)
    entries = []
    for offset in (0, bands):
        def left(i, j, sign):
            if offset == 0:
                return (i, bands + i, j, sign)
            return (bands + i, i, bands + j, -sign)

        entries += complex_entries(0, 0, pairs, lambda i, j: mirrored(i, j, left))
    right = lambda i, j, sign: (i, bands + i, 2 * bands + j, sign)
    return entries + complex_entries(
        0, gram_rows(bands, True), pairs, lambda i, j: mirrored(i, j, right)
    )


def result_entries(bands, width, first_pieces, second_pieces):
    size, own = 2 * bands, pair_list(bands, True)
    every = pair_list(bands, False)

    def spot(matrix, row, column):
        return lambda i, j, sign: (
            2 * size * matrix + row + i, 2 * size * matrix + size + row + i, column + j, sign
        )

    entries = complex_entries(0, 0, own, lambda i, j: mirrored(i, j, spot(0, 0, 0)))
    entries += complex_entries(
        0, gram_rows(bands, True), own, lambda i, j: mirrored(i, j, spot(1, 0, 0))
    )
    source, base = first_pieces, 0
    entries += complex_entries(
        source, base, every,
        lambda i, j: [spot(0, 0, bands)(i, j, 1.0), spot(0, bands, 0)(j, i, -1.0)],
    )
    base += gram_rows(bands, False)
    entries += complex_entries(
        source, base, own, lambda i, j: mirrored(i, j, spot(0, bands, bands))
    )
    base += gram_rows(bands, True)
    entries += complex_entries(
        source, base, every,
        lambda i, j: [spot(1, bands, 0)(i, j, 1.0), spot(1, 0, bands)(j, i, -1.0)],
    )
    source += second_pieces
    for shift in range(bands // 2 + 1):
        for lane in range(width):
            i = lane // (width // bands)
            j = (i - shift) % bands
            places = [(i, j, 1.0)]
            if shift and 2 * shift != bands:
                places.append((j, i, -1.0))
            for row, column, sign in places:
                real_row, imag_row, at, sign = spot(1, bands, bands)(row, column, sign)
                entries.append((source + 2 * shift, lane, real_row, at, 1.0))
                if shift:
                    entries.append((source + 2 * shift + 1, lane, imag_row, at, sign))
    return entries


def solve(system, size, width):
    row_at = lax.broadcasted_iota(jnp.int32, system.shape, 0)
    for k in range(size):
        pivot = system[k : k + 1, :] / system[k : k + 1, k : k + 1]
        system = jnp.where(row_at == k, pivot, system - system[:, k : k + 1] * pivot)
    return system


def wave(length, weight, fraction, indices):
    signed = jnp.where(indices >= length // 2, indices - length, indices).astype(jnp.float32)
    return 2.0 * math.pi / length * (signed + weight * fraction)


class Place:
    def __init__(self, groups, slabs):
        self.groups, self.slabs = groups, slabs
        self.group = lax.axis_index("band")
        self.slab = lax.axis_index("slab")
        self.layer, self.core = self.slab // 2, self.slab % 2
        self.cell = 2 * self.group + self.core

    def slab_peer(self, step):
        slab = lax.rem(self.slab + step, self.slabs)
        return slab, (self.group, slab)

    def band_peer(self, step):
        group = lax.rem(self.group + step, self.groups)
        return group, (group, self.slab)

    def plane_peer(self, step):
        cell = lax.rem(self.cell + step, 2 * self.groups)
        return cell, (cell // 2, 2 * self.layer + cell % 2)


def enter(devices):
    barrier = pltpu.get_barrier_semaphore()
    for device in devices:
        pl.semaphore_signal(barrier, inc=1, device_id=device, device_id_type=MESH)
    pl.semaphore_wait(barrier, len(devices))


def send(source, target, send_sem, recv_sem, device):
    pltpu.make_async_remote_copy(
        src_ref=source,
        dst_ref=target,
        send_sem=send_sem,
        recv_sem=recv_sem,
        device_id=device,
        device_id_type=MESH,
    ).start()


def await_bytes(ref, sem):
    pltpu.make_async_copy(ref, ref, sem).wait()


def total(place, mine, first, second, sems, values):
    mine[0] = values
    first[place.slab] = values
    for step in range(1, place.slabs):
        _, device = place.slab_peer(step)
        send(mine.at[0], first.at[place.slab], sems.at[0], sems.at[1], device)
    await_bytes(first.at[pl.ds(0, place.slabs - 1)], sems.at[1])
    values = first[0]
    for slab in range(1, place.slabs):
        values = values + first[slab]
    mine[1] = values
    second[place.group] = values
    for step in range(1, place.groups):
        _, device = place.band_peer(step)
        send(mine.at[1], second.at[place.group], sems.at[2], sems.at[3], device)
    await_bytes(second.at[pl.ds(0, place.groups - 1)], sems.at[3])
    values = second[0]
    for group in range(1, place.groups):
        values = values + second[group]
    await_bytes(first.at[pl.ds(0, place.slabs - 1)], sems.at[0])
    await_bytes(second.at[pl.ds(0, place.groups - 1)], sems.at[2])
    return values


def lane_sums(tile, acc):
    rows = acc.shape[0]
    tile[...] = jnp.zeros_like(tile)
    tile[:rows, :] = jnp.sum(acc[...], axis=1)
    ones = jnp.ones((8, tile.shape[1]), jnp.float32)
    return lax.dot_general(
        ones, tile[...], (((1,), (1,)), ((), ())), precision=HIGHEST,
        preferred_element_type=jnp.float32,
    )


def step_kernel(
    groups, slabs, solve_sources, result_sources,
    permittivity, bloch, block, materials, x_plus, x_split, x_minus, y_plus, y_minus, z_plus,
    z_minus, solve_spread, solve_gather, result_spread, result_gather,
    search, results,
    work, image, out_y, in_z, out_z, in_y, out_x, eta, local_eta, cells, waves, depths, mixing,
    first_acc, first_tile, first_mine, first_slab, first_band,
    second_acc, field_acc, second_tile, second_mine, second_slab, second_band,
    sems, ends, tail,
):
    place = Place(groups, slabs)
    bands, _, _, depth, rows, width = block.shape
    half = depth // 2
    height = rows * slabs
    length = depth * groups
    share = out_y.shape[3] // half
    cell_count = length * height * width
    step = step_count(half)
    chunks = half // step
    part = step * share

    enter(
        [place.slab_peer(i)[1] for i in range(1, slabs)]
        + [
            (lax.rem(place.group + i, groups), 2 * place.layer + core)
            for i in range(1, groups)
            for core in range(2)
        ]
    )

    @pl.loop(0, chunks)
    def _(k):
        for i in range(1, slabs):
            slab, device = place.slab_peer(i)
            send(
                block.at[slab // 2, :, :, pl.ds(half * (slab % 2) + k * step, step), :, :],
                work.at[:, :, pl.ds(k * step, step), pl.ds(rows * place.slab, rows), :],
                sems.at[0, k], sems.at[1, k], device,
            )

    @pl.loop(0, length // slabs)
    def _(z):
        for cell in range(2 * groups):
            found = materials[z, cell * share : (cell + 1) * share, :]
            values = jnp.zeros(found.shape, jnp.float32)
            for material in range(permittivity.shape[0]):
                values = jnp.where(found == material, permittivity[material] / cell_count, values)
            cells[cell, pl.ds(z * share, share), :] = values

    slab_cells = cells.shape[1]
    for i in range(1, slabs):
        slab, device = place.slab_peer(i)
        send(
            cells.at[2 * place.group + slab % 2],
            eta.at[pl.ds(slab_cells * place.slab, slab_cells), :],
            tail.at[2, 0], tail.at[2, 1], device,
        )
    eta[pl.ds(slab_cells * place.slab, slab_cells), :] = cells[place.cell]

    fraction = (bloch[0].astype(jnp.float32) + 1.0) / KPOINTS
    at_x = lax.broadcasted_iota(jnp.int32, (height, width), 1)
    at_y = lax.broadcasted_iota(jnp.int32, (height, width), 0)
    wave_x, wave_y = wave(width, 0.5, fraction, at_x), wave(height, 0.35, fraction, at_y)
    planar = jnp.sqrt(wave_x * wave_x + wave_y * wave_y)
    waves[0], waves[1], waves[2] = wave_x / planar, wave_y / planar, planar

    @pl.loop(0, depth)
    def _(z):
        at_z = jnp.broadcast_to(place.group * depth + z, (8, width))
        depths[z] = wave(length, 0.2, fraction, at_z)

    first_acc[...] = jnp.zeros_like(first_acc)
    gram(first_acc, 0, True, block, block, depth, lambda t: t)

    @pl.loop(0, chunks)
    def _(k):
        await_bytes(
            work.at[:, :, pl.ds(0, step), pl.ds(0, rows * (slabs - 1)), :], sems.at[1, k]
        )

        @pl.loop(0, step)
        def _(i):
            z = k * step + i
            for comp in range(2):
                for ri in range(2):
                    work[comp, ri, z, pl.ds(rows * place.slab, rows), :] = block[
                        place.layer, comp, ri, half * place.core + z
                    ]
            across, along, planar = waves[0], waves[1], waves[2]
            deep = depths[half * place.core + z, 0:1, :]
            size = jnp.sqrt(planar * planar + deep * deep)
            fields = []
            for ri in range(2):
                one = work[0, ri, z]
                two = work[1, ri, z] * size
                upright = one * deep
                fields.append(
                    [across * upright - along * two, along * upright + across * two, -planar * one]
                )
            curled = jnp.concatenate(
                [jnp.concatenate([fields[0][c], fields[1][c]], 1) for c in range(3)], 0
            )
            lines = right_transform(curled, x_plus)
            stacked = jnp.concatenate(
                [
                    jnp.concatenate(
                        [
                            lines[c * height : (c + 1) * height, :width],
                            lines[c * height : (c + 1) * height, width:],
                        ],
                        0,
                    )
                    for c in range(3)
                ],
                1,
            )
            planes = left_transform(y_plus, stacked)
            for c in range(3):
                for ri in range(2):
                    for cell in range(2 * groups):
                        base = ri * height + cell * share
                        out_y[cell, c, ri, pl.ds(z * share, share), :] = planes[
                            base : base + share, c * width : (c + 1) * width
                        ]

        for i in range(1, 2 * groups):
            cell, device = place.plane_peer(i)
            send(
                out_y.at[cell, :, :, pl.ds(k * part, part), :],
                in_z.at[:, :, pl.ds(place.cell * half * share + k * part, part), :],
                sems.at[2, k], sems.at[3, k], device,
            )
        for c in range(3):
            for ri in range(2):
                in_z[c, ri, pl.ds(place.cell * half * share + k * part, part), :] = out_y[
                    place.cell, c, ri, pl.ds(k * part, part), :
                ]

    await_bytes(eta.at[pl.ds(0, slab_cells * (slabs - 1)), :], tail.at[2, 1])

    @pl.loop(0, chunks)
    def _(k):
        await_bytes(in_z.at[:, :, pl.ds(0, part * (2 * groups - 1)), :], sems.at[3, k])

    @pl.loop(0, share // 2)
    def _(pair):
        weights = [eta[pl.ds(2 * pair + j, length, stride=share), :] for j in range(2)]
        for c in range(3):
            stacked = jnp.concatenate(
                [
                    jnp.concatenate(
                        [in_z[c, ri, pl.ds(2 * pair + j, length, stride=share), :] for ri in range(2)],
                        0,
                    )
                    for j in range(2)
                ],
                1,
            )
            field = left_transform(z_plus, stacked)
            weight = jnp.concatenate(weights, 1)
            field = field * jnp.concatenate([weight, weight], 0)
            back = left_transform(z_minus, field)
            for j in range(2):
                for ri in range(2):
                    out_z[c, ri, pl.ds(2 * pair + j, length, stride=share), :] = back[
                        ri * length : (ri + 1) * length, j * width : (j + 1) * width
                    ]

    @pl.loop(0, chunks)
    def _(k):
        for i in range(1, 2 * groups):
            cell, device = place.plane_peer(i)
            send(
                out_z.at[:, :, pl.ds(cell * half * share + k * part, part), :],
                in_y.at[place.cell, :, :, pl.ds(k * part, part), :],
                sems.at[4, k], sems.at[5, k], device,
            )

    @pl.loop(0, chunks)
    def _(k):
        for c in range(3):
            for ri in range(2):
                in_y[place.cell, c, ri, pl.ds(k * part, part), :] = out_z[
                    c, ri, pl.ds(place.cell * half * share + k * part, part), :
                ]
        await_bytes(
            in_y.at[pl.ds(0, 2 * groups - 1), :, :, pl.ds(0, part), :], sems.at[5, k]
        )

        @pl.loop(0, step)
        def _(i):
            z = k * step + i
            stacked = jnp.concatenate(
                [
                    jnp.concatenate(
                        [
                            in_y[cell, c, ri, pl.ds(z * share, share), :]
                            for ri in range(2)
                            for cell in range(2 * groups)
                        ],
                        0,
                    )
                    for c in range(3)
                ],
                1,
            )
            planes = left_transform(y_minus, stacked)
            lines = jnp.concatenate(
                [
                    jnp.concatenate(
                        [
                            planes[:height, c * width : (c + 1) * width],
                            planes[height:, c * width : (c + 1) * width],
                        ],
                        1,
                    )
                    for c in range(3)
                ],
                0,
            )
            curled = right_transform(lines, x_minus)
            across, along, planar = waves[0], waves[1], waves[2]
            deep = depths[half * place.core + z, 0:1, :]
            size = jnp.sqrt(planar * planar + deep * deep)
            for ri in range(2):
                fields = [
                    curled[c * height : (c + 1) * height, ri * width : (ri + 1) * width]
                    for c in range(3)
                ]
                work[0, ri, z] = deep * (across * fields[0] + along * fields[1]) - planar * fields[2]
                work[1, ri, z] = size * (across * fields[1] - along * fields[0])
            for comp in range(2):
                for ri in range(2):
                    image[place.layer, comp, ri, half * place.core + z] = work[
                        comp, ri, z, pl.ds(rows * place.slab, rows), :
                    ]

        for i in range(1, slabs):
            slab, device = place.slab_peer(i)
            send(
                work.at[:, :, pl.ds(k * step, step), pl.ds(rows * slab, rows), :],
                image.at[place.layer, :, :, pl.ds(half * place.core + k * step, step), :, :],
                sems.at[6, k], sems.at[7, k], device,
            )

    @pl.loop(0, chunks)
    def _(k):
        await_bytes(
            work.at[:, :, pl.ds(0, step), pl.ds(0, rows * (slabs - 1)), :], sems.at[7, k]
        )
        gram(
            first_acc, gram_rows(bands, True), True, block, image, 2 * step,
            lambda t: half * (t // step) + k * step + t % step,
        )

    first_sums = total(place, first_mine, first_slab, first_band, tail.at[0], lane_sums(first_tile, first_acc))
    pieces = lambda values, row: [
        values[row : row + 1, at : at + width] for at in range(0, values.shape[1], width)
    ]
    system = solve(
        scatter(pieces(first_sums, 0), solve_sources, solve_spread, solve_gather), 2 * bands, width
    )
    for row in range(2 * bands):
        for j in range(bands):
            mixing[row, j] = jnp.broadcast_to(
                system[row : row + 1, 2 * bands + j : 2 * bands + j + 1], (8, width)
            )

    @pl.loop(0, chunks)
    def _(k):
        slab_bytes = work.at[:, :, pl.ds(0, step), pl.ds(0, rows * (slabs - 1)), :]
        plane_bytes = in_z.at[:, :, pl.ds(0, part * (2 * groups - 1)), :]
        await_bytes(slab_bytes, sems.at[0, k])
        await_bytes(plane_bytes, sems.at[2, k])
        await_bytes(plane_bytes, sems.at[4, k])
        await_bytes(slab_bytes, sems.at[6, k])

    await_bytes(eta.at[pl.ds(0, slab_cells * (slabs - 1)), :], tail.at[2, 0])

    parts = rows // 8
    thin = length // slabs
    quarter = width // groups
    second_acc[...] = jnp.zeros_like(second_acc)
    field_acc[...] = jnp.zeros_like(field_acc)
    lane = lax.broadcasted_iota(jnp.int32, (1, width), 1) // quarter
    deep_step = 8 if depth % 8 == 0 else 1

    @pl.loop(0, parts)
    def _(part):
        band_rows = pl.ds(part * 8, 8)
        across, along, planar = (
            waves[i, pl.ds(rows * place.slab + part * 8, 8), :] for i in range(3)
        )

        @pl.loop(0, depth)
        def _(z):
            tile_at = (z, band_rows, slice(None))
            deep = depths[z]
            scale = 1.0 / (planar * planar + deep * deep + 1.0)
            for comp in range(2):
                reals = [block[(i, comp, 0) + tile_at] for i in range(bands)]
                imags = [block[(i, comp, 1) + tile_at] for i in range(bands)]
                for j in range(bands):
                    real = image[(j, comp, 0) + tile_at]
                    imag = image[(j, comp, 1) + tile_at]
                    for i in range(bands):
                        real = real - (reals[i] * mixing[i, j] - imags[i] * mixing[bands + i, j])
                        imag = imag - (reals[i] * mixing[bands + i, j] + imags[i] * mixing[i, j])
                    search[(j, comp, 0) + tile_at] = real * scale
                    search[(j, comp, 1) + tile_at] = imag * scale

        @pl.loop(0, depth // deep_step)
        def _(group):
            planes = pl.ds(group * deep_step, deep_step)
            deep = depths[planes]
            size = jnp.sqrt(planar * planar + deep * deep)
            count = deep_step * 8
            lines = []
            for i in range(bands):
                fields = []
                for ri in range(2):
                    one = search[i, 0, ri, planes, band_rows, :]
                    two = search[i, 1, ri, planes, band_rows, :] * size
                    upright = one * deep
                    fields.append(
                        [
                            value.reshape(count, width)
                            for value in (
                                across * upright - along * two,
                                along * upright + across * two,
                                -planar * one,
                            )
                        ]
                    )
                curled = jnp.concatenate(
                    [jnp.concatenate([fields[0][c], fields[1][c]], 1) for c in range(3)], 0
                )
                lines.append(right_transform(curled, x_split.at[i]))
            at = pl.ds(group * count, count)
            for target in range(groups):
                for ri in range(2):
                    columns = slice(ri * width, (ri + 1) * width)
                    packed = lines[(-target) % groups][:, columns]
                    for spot in range(1, groups):
                        packed = jnp.where(
                            lane == spot, lines[(spot - target) % groups][:, columns], packed
                        )
                    for c in range(3):
                        out_x[part * groups + target, c, ri, at, :] = packed[c * count : (c + 1) * count]

        for c in range(3):
            for i in range(1, groups):
                group, device = place.band_peer(i)
                send(
                    out_x.at[part * groups + group, c],
                    in_z.at[c, :, pl.ds((part * length + depth * place.group) * 8, depth * 8), :],
                    ends.at[0, part * 3 + c], ends.at[1, part * 3 + c], device,
                )
            for ri in range(2):
                in_z[c, ri, pl.ds((part * length + depth * place.group) * 8, depth * 8), :] = out_x[
                    part * groups + place.group, c, ri
                ]

    @pl.loop(0, 3 * parts)
    def _(k):
        part, c = k // 3, k % 3
        await_bytes(in_z.at[c, :, pl.ds(0, depth * 8 * (groups - 1)), :], ends.at[1, k])
        base = part * length * 8

        @pl.loop(0, 4)
        def _(pair):
            stacked = jnp.concatenate(
                [
                    jnp.concatenate(
                        [
                            in_z[c, ri, pl.ds(base + 2 * pair + j, length, stride=8), :]
                            for ri in range(2)
                        ],
                        0,
                    )
                    for j in range(2)
                ],
                1,
            )
            columns = left_transform(z_plus, stacked)
            for j in range(2):
                for ri in range(2):
                    out_z[c, ri, pl.ds(base + 2 * pair + j, length, stride=8), :] = columns[
                        ri * length : (ri + 1) * length, j * width : (j + 1) * width
                    ]

        for i in range(1, slabs):
            slab, device = place.slab_peer(i)
            send(
                out_z.at[c, :, pl.ds(base + thin * 8 * slab, thin * 8), :],
                in_y.at[place.slab, c, :, pl.ds(part * thin * 8, thin * 8), :],
                ends.at[2, k], ends.at[3, k], device,
            )
        for ri in range(2):
            in_y[place.slab, c, ri, pl.ds(part * thin * 8, thin * 8), :] = out_z[
                c, ri, pl.ds(base + thin * 8 * place.slab, thin * 8), :
            ]

    @pl.loop(0, thin)
    def _(z):
        for cell in range(2 * groups):
            values = cells[cell, pl.ds(z * share, share), :]
            values = pltpu.roll(values, lax.rem(width - quarter * place.group, width), 1)
            values = jnp.where(lane == 0, values, 0.0)
            reach = quarter
            while reach < width:
                values = values + pltpu.roll(values, reach, 1)
                reach *= 2
            local_eta[z, cell * share : (cell + 1) * share, :] = values

    base = gram(second_acc, 0, False, block, search, depth, lambda t: t)
    base = gram(second_acc, base, True, search, search, depth, lambda t: t)
    gram(second_acc, base, False, search, image, depth, lambda t: t)

    for c in range(3):
        for part in range(parts):
            await_bytes(
                in_y.at[pl.ds(0, slabs - 1), c, :, pl.ds(0, thin * 8), :],
                ends.at[3, part * 3 + c],
            )

        @pl.loop(0, thin)
        def _(z, c=c):
            stacked = jnp.concatenate(
                [
                    in_y[slab, c, ri, pl.ds(part * thin * 8 + 8 * z, 8), :]
                    for ri in range(2)
                    for slab in range(slabs)
                    for part in range(parts)
                ],
                0,
            )
            field = left_transform(y_plus, stacked)
            real, imag = field[:height], field[height:]
            weight = local_eta[z]
            real_weighted, imag_weighted = real * weight, imag * weight
            for shift in range(bands // 2 + 1):
                if shift == 0:
                    real_other, imag_other = real, imag
                else:
                    real_other = pltpu.roll(real, quarter * shift, 1)
                    imag_other = pltpu.roll(imag, quarter * shift, 1)
                real_term = real_weighted * real_other + imag_weighted * imag_other
                imag_term = real_weighted * imag_other - imag_weighted * real_other
                for place_of, term in ((2 * shift, real_term), (2 * shift + 1, imag_term)):
                    field_acc[place_of] += jnp.sum(term.reshape(height // 8, 8, width), axis=0)

    fields = jnp.sum(field_acc[...], axis=1)
    fields = pltpu.roll(fields, lax.rem(width - quarter * place.group, width), 1)
    values = lane_sums(second_tile, second_acc)
    if values.shape[1] > width:
        empty = jnp.zeros((fields.shape[0], values.shape[1] - width), jnp.float32)
        fields = jnp.concatenate([fields, empty], 1)
    second_sums = total(
        place, second_mine, second_slab, second_band, tail.at[1],
        jnp.concatenate([values, fields], 0),
    )
    listed = pieces(first_sums, 0) + pieces(second_sums, 0)
    for row in range(2 * (bands // 2 + 1)):
        listed.append(second_sums[8 + row : 9 + row, :width])
    results[...] = scatter(listed, result_sources, result_spread, result_gather) / cell_count

    @pl.loop(0, 3 * parts)
    def _(k):
        await_bytes(in_z.at[0, :, pl.ds(0, depth * 8 * (groups - 1)), :], ends.at[0, k])
        await_bytes(in_y.at[pl.ds(0, slabs - 1), 0, :, pl.ds(0, thin * 8), :], ends.at[2, k])


def vmem(count):
    return [pl.BlockSpec(memory_space=pltpu.VMEM)] * count


def round_up(value, step):
    return -(-value // step) * step


def step(block, materials, permittivity, bloch, groups, slabs):
    bands, _, _, depth, rows, width = block.shape
    half, height, length = depth // 2, rows * slabs, depth * groups
    share = height // (2 * groups)
    thin, parts, quarter = length // slabs, rows // 8, width // groups
    chunks = half // step_count(half)
    first_count = 2 * gram_rows(bands, True)
    first_lanes = round_up(first_count, width)
    second_count = 2 * gram_rows(bands, False) + gram_rows(bands, True)
    second_lanes = round_up(second_count, width)
    field_rows = round_up(2 * (bands // 2 + 1), 8)
    message = (8 + field_rows, second_lanes)

    plain = dft_matrix(width, 1.0).T
    orders = []
    for band in range(bands):
        spots = np.arange(width) // quarter
        source = ((spots - band) % groups) * quarter + np.arange(width) % quarter
        orders.append(right_table(plain[:, np.concatenate([source, width + source])]))
    first_pieces, second_pieces = first_lanes // width, second_lanes // width
    solve_sources, *solve_tables = scatter_tables(system_entries(bands), first_pieces, width)
    result_sources, *result_tables = scatter_tables(
        result_entries(bands, width, first_pieces, second_pieces),
        first_pieces + second_pieces + 2 * (bands // 2 + 1),
        width,
    )
    tables = [
        right_table(plain),
        np.stack(orders),
        right_table(dft_matrix(width, -1.0).T),
        left_table(height, 1.0),
        left_table(height, -1.0),
        left_table(length, 1.0),
        left_table(length, -1.0),
        *solve_tables,
        *result_tables,
    ]
    single = lambda *shape: pltpu.VMEM(shape, jnp.float32)
    by_cell = (2 * groups, 3, 2, half * share, width)
    by_part = (parts * groups, 3, 2, depth * 8, width)
    out_x = [] if by_cell == by_part else [single(*by_part)]
    kernel = partial(step_kernel, groups, slabs, solve_sources, result_sources)

    def body(*refs):
        refs = list(refs)
        if not out_x:
            outgoing = 2 + 2 + len(tables) + 2 + 2
            refs.insert(outgoing + 4, refs[outgoing])
        kernel(*refs)

    return pl.pallas_call(
        body,
        in_specs=[pl.BlockSpec(memory_space=pltpu.SMEM)] * 2 + vmem(2 + len(tables)),
        out_specs=vmem(2),
        out_shape=[
            jax.ShapeDtypeStruct(block.shape, jnp.float32),
            jax.ShapeDtypeStruct((result_tables[0].shape[0], width), jnp.float32),
        ],
        scratch_shapes=[
            single(2, 2, half, height, width),
            single(*block.shape),
            single(*by_cell),
            single(3, 2, length * share, width),
            single(3, 2, length * share, width),
            single(*by_cell),
            *out_x,
            single(length * share, width),
            single(thin, height, width),
            single(2 * groups, thin * share, width),
            single(3, height, width),
            single(depth, 8, width),
            single(2 * bands, bands, 8, width),
            single(first_count, 8, width),
            single(first_lanes, width),
            single(2, 8, first_lanes),
            single(slabs, 8, first_lanes),
            single(groups, 8, first_lanes),
            single(second_count, 8, width),
            single(field_rows, 8, width),
            single(second_lanes, width),
            single(2, *message),
            single(slabs, *message),
            single(groups, *message),
            pltpu.SemaphoreType.DMA((8, chunks)),
            pltpu.SemaphoreType.DMA((4, 3 * parts)),
            pltpu.SemaphoreType.DMA((3, 4)),
        ],
        compiler_params=pltpu.CompilerParams(
            collective_id=0, has_side_effects=True, vmem_limit_bytes=VMEM_LIMIT
        ),
    )(permittivity, bloch, block, materials, *[jnp.asarray(table) for table in tables])


def shards(band_block, material_grid, inverse_permittivity, bloch_index):
    groups, slabs = lax.axis_size("band"), lax.axis_size("slab")
    size = 2 * band_block.shape[0]
    search_block, results = step(
        band_block, material_grid, inverse_permittivity, bloch_index, groups, slabs
    )
    results = results[:, :size].reshape(2, 2, size, size)
    return (search_block, results[0], results[1])


def solution(mesh):
    return jax.shard_map(
        shards,
        mesh=mesh,
        in_specs=(P(None, None, None, "band", "slab", None), P("slab", None, None), P(), P()),
        out_specs=(P(None, None, None, "band", "slab", None), P(), P()),
        check_vma=False,
    )
```

```python
from functools import partial
import math

import jax
import jax.numpy as jnp
import numpy as np
from jax import lax
from jax.experimental import pallas as pl
from jax.experimental.pallas import tpu as pltpu
from jax.sharding import PartitionSpec as P

KPOINTS = 8
HIGHEST = lax.Precision.HIGHEST
MESH = pl.DeviceIdType.MESH
VMEM_LIMIT = 54 * 1024 * 1024
WINDOW = 3


def halves(values):
    high = values.astype(jnp.bfloat16)
    return high, (values - high.astype(jnp.float32)).astype(jnp.bfloat16)


def dft_matrix(length, direction):
    indices = np.arange(length)
    angles = 2.0 * np.pi / length * (np.outer(indices, indices) % length)
    cosine, sine = np.cos(angles), direction * np.sin(angles)
    return np.block([[cosine, -sine], [sine, cosine]])


def numpy_halves(matrix):
    single = matrix.astype(np.float32)
    high = single.astype(jnp.bfloat16)
    low = (single - high.astype(np.float32)).astype(jnp.bfloat16)
    return high, low


def left_table(length, direction):
    return np.concatenate(numpy_halves(dft_matrix(length, direction)), 0)


def right_table(matrix):
    high, low = numpy_halves(matrix)
    return np.concatenate([high, high, low], 0)


def dot(left, right):
    return jnp.dot(left, right, preferred_element_type=jnp.float32)


def left_transform(table, values):
    size = values.shape[0]
    high, low = halves(values)
    main = dot(table[...], high)
    rest = dot(table[:size, :], low)
    return main[:size] + (main[size:] + rest)


def right_transform(values, table):
    high, low = halves(values)
    return dot(jnp.concatenate([high, low, high], 1), table[...])


def gram(acc, base, hermitian, left, right, count, depth_of):
    bands, rows, lanes = left.shape[0], left.shape[4], left.shape[5]
    for i in range(bands):
        others = list(range(i if hermitian else 0, bands))

        def body(step, sums, i=i, others=others):
            depth = depth_of(step)
            sums = list(sums)
            for row in range(0, rows, 8):
                tile = (depth, pl.ds(row, 8), slice(None))
                for comp in range(2):
                    left_real = left[(i, comp, 0) + tile]
                    left_imag = left[(i, comp, 1) + tile]
                    for place, j in enumerate(others):
                        right_real = right[(j, comp, 0) + tile]
                        right_imag = right[(j, comp, 1) + tile]
                        sums[2 * place] += left_real * right_real + left_imag * right_imag
                        sums[2 * place + 1] += left_real * right_imag - left_imag * right_real
            return tuple(sums)

        zeros = tuple(jnp.zeros((8, lanes), jnp.float32) for _ in range(2 * len(others)))
        sums = lax.fori_loop(0, count, body, zeros)
        for place, value in enumerate(sums):
            acc[base + place] += value
        base += 2 * len(others)
    return base


def gram_rows(bands, hermitian):
    return bands * (bands + 1) if hermitian else 2 * bands * bands


def scatter_tables(entries, pieces, width):
    slots = {}
    rows = 8 * (-(-(1 + max(entry[2] for entry in entries)) // 8))
    for source, lane, row, column, sign in entries:
        columns = slots.setdefault((source, lane), {})
        columns.setdefault(column, {})[row] = sign
    blocks = []
    for source in range(pieces):
        depth = max([len(v) for (s, _), v in slots.items() if s == source], default=0)
        blocks += [(source, place) for place in range(depth)]
    spread = np.zeros((rows, width * len(blocks)), np.float32)
    gather = np.zeros((width * len(blocks), width), np.float32)
    for index, (source, place) in enumerate(blocks):
        for lane in range(width):
            columns = list(slots.get((source, lane), {}).items())
            if place < len(columns):
                column, signs = columns[place]
                gather[index * width + lane, column] = 1.0
                for row, sign in signs.items():
                    spread[row, index * width + lane] = sign
    return [source for source, _ in blocks], spread, gather.astype(jnp.bfloat16)


def scatter(values, sources, spread, gather):
    rows, width = spread.shape[0], values[0].shape[1]
    spots = jnp.concatenate(
        [
            jnp.broadcast_to(values[source], (rows, width))
            * spread[:, place * width : (place + 1) * width]
            for place, source in enumerate(sources)
        ],
        1,
    )
    high, rest = halves(spots)
    low = (spots - high.astype(jnp.float32)) - rest.astype(jnp.float32)
    return (dot(high, gather[...]) + dot(rest, gather[...])) + dot(
        low.astype(jnp.bfloat16), gather[...]
    )


def pair_list(bands, hermitian):
    return [(i, j) for i in range(bands) for j in range(i if hermitian else 0, bands)]


def complex_entries(source, base, pairs, put):
    entries = []
    for place, (i, j) in enumerate(pairs):
        for real_row, imag_row, column, sign in put(i, j):
            lane = base + 2 * place
            entries.append((source + lane // 128, lane % 128, real_row, column, 1.0))
            entries.append((source + (lane + 1) // 128, (lane + 1) % 128, imag_row, column, sign))
    return entries


def mirrored(i, j, put):
    return [put(i, j, 1.0)] if i == j else [put(i, j, 1.0), put(j, i, -1.0)]


def system_entries(bands):
    pairs = pair_list(bands, True)
    entries = []
    for offset in (0, bands):
        def left(i, j, sign):
            if offset == 0:
                return (i, bands + i, j, sign)
            return (bands + i, i, bands + j, -sign)

        entries += complex_entries(0, 0, pairs, lambda i, j: mirrored(i, j, left))
    right = lambda i, j, sign: (i, bands + i, 2 * bands + j, sign)
    return entries + complex_entries(
        0, gram_rows(bands, True), pairs, lambda i, j: mirrored(i, j, right)
    )


def result_entries(bands, width, first_pieces, second_pieces):
    size, own = 2 * bands, pair_list(bands, True)
    every = pair_list(bands, False)

    def spot(matrix, row, column):
        return lambda i, j, sign: (
            2 * size * matrix + row + i, 2 * size * matrix + size + row + i, column + j, sign
        )

    entries = complex_entries(0, 0, own, lambda i, j: mirrored(i, j, spot(0, 0, 0)))
    entries += complex_entries(
        0, gram_rows(bands, True), own, lambda i, j: mirrored(i, j, spot(1, 0, 0))
    )
    source, base = first_pieces, 0
    entries += complex_entries(
        source, base, every,
        lambda i, j: [spot(0, 0, bands)(i, j, 1.0), spot(0, bands, 0)(j, i, -1.0)],
    )
    base += gram_rows(bands, False)
    entries += complex_entries(
        source, base, own, lambda i, j: mirrored(i, j, spot(0, bands, bands))
    )
    base += gram_rows(bands, True)
    entries += complex_entries(
        source, base, every,
        lambda i, j: [spot(1, bands, 0)(i, j, 1.0), spot(1, 0, bands)(j, i, -1.0)],
    )
    source += second_pieces
    for shift in range(bands // 2 + 1):
        for lane in range(width):
            i = lane // (width // bands)
            j = (i - shift) % bands
            places = [(i, j, 1.0)]
            if shift and 2 * shift != bands:
                places.append((j, i, -1.0))
            for row, column, sign in places:
                real_row, imag_row, at, sign = spot(1, bands, bands)(row, column, sign)
                entries.append((source + 2 * shift, lane, real_row, at, 1.0))
                if shift:
                    entries.append((source + 2 * shift + 1, lane, imag_row, at, sign))
    return entries


def solve(system, size, width):
    row_at = lax.broadcasted_iota(jnp.int32, system.shape, 0)
    for k in range(size):
        pivot = system[k : k + 1, :] / system[k : k + 1, k : k + 1]
        system = jnp.where(row_at == k, pivot, system - system[:, k : k + 1] * pivot)
    return system


def wave(length, weight, fraction, indices):
    signed = jnp.where(indices >= length // 2, indices - length, indices).astype(jnp.float32)
    return 2.0 * math.pi / length * (signed + weight * fraction)


class Place:
    def __init__(self, groups, slabs):
        self.groups, self.slabs = groups, slabs
        self.group = lax.axis_index("band")
        self.slab = lax.axis_index("slab")
        self.layer, self.core = self.slab // 2, self.slab % 2
        self.cell = 2 * self.group + self.core

    def slab_peer(self, step):
        slab = lax.rem(self.slab + step, self.slabs)
        return slab, (self.group, slab)

    def band_peer(self, step):
        group = lax.rem(self.group + step, self.groups)
        return group, (group, self.slab)

    def plane_peer(self, step):
        cell = lax.rem(self.cell + step, 2 * self.groups)
        return cell, (cell // 2, 2 * self.layer + cell % 2)


def enter(devices):
    barrier = pltpu.get_barrier_semaphore()
    for device in devices:
        pl.semaphore_signal(barrier, inc=1, device_id=device, device_id_type=MESH)
    pl.semaphore_wait(barrier, len(devices))


def send(source, target, send_sem, recv_sem, device):
    pltpu.make_async_remote_copy(
        src_ref=source,
        dst_ref=target,
        send_sem=send_sem,
        recv_sem=recv_sem,
        device_id=device,
        device_id_type=MESH,
    ).start()


def await_bytes(ref, sem):
    pltpu.make_async_copy(ref, ref, sem).wait()


def total(place, mine, first, second, sems, values):
    mine[0] = values
    first[place.slab] = values
    for step in range(1, place.slabs):
        _, device = place.slab_peer(step)
        send(mine.at[0], first.at[place.slab], sems.at[0], sems.at[1], device)
    await_bytes(first.at[pl.ds(0, place.slabs - 1)], sems.at[1])
    values = first[0]
    for slab in range(1, place.slabs):
        values = values + first[slab]
    mine[1] = values
    second[place.group] = values
    for step in range(1, place.groups):
        _, device = place.band_peer(step)
        send(mine.at[1], second.at[place.group], sems.at[2], sems.at[3], device)
    await_bytes(second.at[pl.ds(0, place.groups - 1)], sems.at[3])
    values = second[0]
    for group in range(1, place.groups):
        values = values + second[group]
    await_bytes(first.at[pl.ds(0, place.slabs - 1)], sems.at[0])
    await_bytes(second.at[pl.ds(0, place.groups - 1)], sems.at[2])
    return values


def lane_sums(tile, acc):
    rows = acc.shape[0]
    tile[...] = jnp.zeros_like(tile)
    tile[:rows, :] = jnp.sum(acc[...], axis=1)
    ones = jnp.ones((8, tile.shape[1]), jnp.float32)
    return lax.dot_general(
        ones, tile[...], (((1,), (1,)), ((), ())), precision=HIGHEST,
        preferred_element_type=jnp.float32,
    )


def step_kernel(
    groups, slabs, arrays, solve_sources, result_sources,
    permittivity, bloch, given, *refs,
):
    outside, refs = (given, *refs[: arrays - 1]), refs[arrays - 1 :]
    (search, results), inside, refs = refs[:2], refs[2 : arrays + 2], refs[arrays + 2 :]
    block, materials, x_split, x_minus, y_plus, y_minus = inside[:6]
    z_plus, z_minus = inside[6:8] if arrays == 12 else (y_plus, y_minus)
    solve_spread, solve_gather, result_spread, result_gather = inside[-4:]
    (
        work, image, out_y, in_z, out_z, in_y, out_x, eta, local_eta, cells, waves, depths, mixing,
        first_acc, first_tile, first_mine, first_slab, first_band,
        second_acc, field_acc, second_tile, second_mine, second_slab, second_band,
        sems, comes, ends, tail, loads,
    ) = refs
    place = Place(groups, slabs)
    bands, _, _, depth, rows, width = block.shape
    half = depth // 2
    height = rows * slabs
    length = depth * groups
    share = out_y.shape[3] // half
    cell_count = length * height * width
    thin = length // slabs
    chunks = half
    parts = share // 8
    lead = min(WINDOW, chunks)

    enter(
        [place.slab_peer(i)[1] for i in range(1, slabs)]
        + [
            (lax.rem(place.group + i, groups), 2 * place.layer + core)
            for i in range(1, groups)
            for core in range(2)
        ]
    )

    for place_of, (source, target) in enumerate(zip(outside, inside)):
        pltpu.make_async_copy(source, target, loads.at[place_of]).start()

    def send_out(k):
        for i in range(1, slabs):
            slab, device = place.slab_peer(i)
            send(
                given.at[slab // 2, :, :, pl.ds(half * (slab % 2) + k, 1), :, :],
                work.at[:, :, pl.ds(k, 1), pl.ds(rows * place.slab, rows), :],
                sems.at[0, k], sems.at[1, k], device,
            )

    @pl.loop(0, lead)
    def _(k):
        send_out(k)

    for place_of, (source, target) in enumerate(zip(outside, inside)):
        pltpu.make_async_copy(source, target, loads.at[place_of]).wait()

    @pl.loop(0, thin)
    def _(z):
        for cell in range(2 * groups):
            for part in range(parts):
                found = materials[z, pl.ds(cell * share + part * 8, 8), :]
                values = jnp.zeros(found.shape, jnp.float32)
                for material in range(permittivity.shape[0]):
                    values = jnp.where(found == material, permittivity[material] / cell_count, values)
                cells[cell, pl.ds((part * thin + z) * 8, 8), :] = values

    def send_cells():
        for part in range(parts):
            target = pl.ds((part * length + thin * place.slab) * 8, thin * 8)
            for i in range(1, slabs):
                slab, device = place.slab_peer(i)
                send(
                    cells.at[2 * place.group + slab % 2, pl.ds(part * thin * 8, thin * 8), :],
                    eta.at[target, :],
                    tail.at[2, part], tail.at[3, part], device,
                )

    for part in range(parts):
        target = pl.ds((part * length + thin * place.slab) * 8, thin * 8)
        eta[target, :] = cells[place.cell, pl.ds(part * thin * 8, thin * 8), :]

    fraction = (bloch[0].astype(jnp.float32) + 1.0) / KPOINTS
    at_x = lax.broadcasted_iota(jnp.int32, (height, width), 1)
    at_y = lax.broadcasted_iota(jnp.int32, (height, width), 0)
    wave_x, wave_y = wave(width, 0.5, fraction, at_x), wave(height, 0.35, fraction, at_y)
    planar = jnp.sqrt(wave_x * wave_x + wave_y * wave_y)
    waves[0], waves[1], waves[2] = wave_x / planar, wave_y / planar, planar

    @pl.loop(0, depth)
    def _(z):
        at_z = jnp.broadcast_to(place.group * depth + z, (8, width))
        depths[z] = wave(length, 0.2, fraction, at_z)

    first_acc[...] = jnp.zeros_like(first_acc)
    gram(first_acc, 0, True, block, block, depth, lambda t: t)

    @pl.loop(0, chunks)
    def _(z):
        await_bytes(
            work.at[:, :, pl.ds(0, 1), pl.ds(0, rows * (slabs - 1)), :], sems.at[1, z]
        )

        @pl.when(z + lead < chunks)
        def _():
            send_out(z + lead)

        @pl.when(z == chunks - 1)
        def _():
            send_cells()

        for comp in range(2):
            for ri in range(2):
                work[comp, ri, z, pl.ds(rows * place.slab, rows), :] = block[
                    place.layer, comp, ri, half * place.core + z
                ]
        across, along, planar = waves[0], waves[1], waves[2]
        deep = depths[half * place.core + z, 0:1, :]
        size = jnp.sqrt(planar * planar + deep * deep)
        fields = []
        for ri in range(2):
            one = work[0, ri, z]
            two = work[1, ri, z] * size
            upright = one * deep
            fields.append(
                [across * upright - along * two, along * upright + across * two, -planar * one]
            )
        curled = jnp.concatenate(
            [jnp.concatenate([fields[0][c], fields[1][c]], 1) for c in range(3)], 0
        )
        lines = right_transform(curled, x_split.at[0])
        stacked = jnp.concatenate(
            [
                jnp.concatenate(
                    [
                        lines[c * height : (c + 1) * height, :width],
                        lines[c * height : (c + 1) * height, width:],
                    ],
                    0,
                )
                for c in range(3)
            ],
            1,
        )
        planes = left_transform(y_plus, stacked)
        for c in range(3):
            for ri in range(2):
                for cell in range(2 * groups):
                    for part in range(parts):
                        base = ri * height + cell * share + part * 8
                        out_y[cell, c, ri, pl.ds((part * half + z) * 8, 8), :] = planes[
                            base : base + 8, c * width : (c + 1) * width
                        ]

        for part in range(parts):
            source = pl.ds((part * half + z) * 8, 8)
            target = pl.ds((part * length + place.cell * half + z) * 8, 8)
            for i in range(1, 2 * groups):
                cell, device = place.plane_peer(i)
                send(
                    out_y.at[cell, :, :, source, :],
                    in_z.at[:, :, target, :],
                    sems.at[2, z], comes.at[part, z], device,
                )
            for c in range(3):
                for ri in range(2):
                    in_z[c, ri, target, :] = out_y[place.cell, c, ri, source, :]

    def columns_of(source, c, first):
        return jnp.concatenate(
            [
                jnp.concatenate(
                    [source[c, ri, pl.ds(first + j, length, stride=8), :] for ri in range(2)], 0
                )
                for j in range(2)
            ],
            1,
        )

    def keep_columns(target, c, first, values):
        for j in range(2):
            for ri in range(2):
                target[c, ri, pl.ds(first + j, length, stride=8), :] = values[
                    ri * length : (ri + 1) * length, j * width : (j + 1) * width
                ]

    for part in range(parts):
        @pl.loop(0, chunks)
        def _(k, part=part):
            await_bytes(in_z.at[:, :, pl.ds(0, 8 * (2 * groups - 1)), :], comes.at[part, k])

        @pl.loop(0, 4)
        def _(pair, part=part):
            first = part * length * 8 + 2 * pair
            for c in range(3):
                keep_columns(in_z, c, first, left_transform(z_plus, columns_of(in_z, c, first)))

    def send_back(k, part):
        for i in range(1, 2 * groups):
            cell, device = place.plane_peer(i)
            send(
                out_z.at[:, :, pl.ds((part * length + cell * half + k) * 8, 8), :],
                in_y.at[place.cell, :, :, pl.ds((part * half + k) * 8, 8), :],
                sems.at[4, k], sems.at[5, k], device,
            )

    for part in range(parts):
        await_bytes(eta.at[pl.ds(0, thin * 8 * (slabs - 1)), :], tail.at[3, part])

        @pl.loop(0, 4)
        def _(pair, part=part):
            first = part * length * 8 + 2 * pair
            weight = jnp.concatenate(
                [eta[pl.ds(first + j, length, stride=8), :] for j in range(2)], 1
            )
            weight = jnp.concatenate([weight, weight], 0)
            for c in range(3):
                field = columns_of(in_z, c, first) * weight
                keep_columns(out_z, c, first, left_transform(z_minus, field))

        @pl.loop(0, lead)
        def _(k, part=part):
            send_back(k, part)

    @pl.loop(0, chunks)
    def _(z):
        for c in range(3):
            for ri in range(2):
                for part in range(parts):
                    in_y[place.cell, c, ri, pl.ds((part * half + z) * 8, 8), :] = out_z[
                        c, ri, pl.ds((part * length + place.cell * half + z) * 8, 8), :
                    ]
        await_bytes(in_y.at[pl.ds(0, 2 * groups - 1), :, :, pl.ds(0, share), :], sems.at[5, z])

        @pl.when(z + lead < chunks)
        def _():
            for part in range(parts):
                send_back(z + lead, part)


        stacked = jnp.concatenate(
            [
                jnp.concatenate(
                    [
                        in_y[cell, c, ri, pl.ds((part * half + z) * 8, 8), :]
                        for ri in range(2)
                        for cell in range(2 * groups)
                        for part in range(parts)
                    ],
                    0,
                )
                for c in range(3)
            ],
            1,
        )
        planes = left_transform(y_minus, stacked)
        lines = jnp.concatenate(
            [
                jnp.concatenate(
                    [
                        planes[:height, c * width : (c + 1) * width],
                        planes[height:, c * width : (c + 1) * width],
                    ],
                    1,
                )
                for c in range(3)
            ],
            0,
        )
        curled = right_transform(lines, x_minus)
        across, along, planar = waves[0], waves[1], waves[2]
        deep = depths[half * place.core + z, 0:1, :]
        size = jnp.sqrt(planar * planar + deep * deep)
        for ri in range(2):
            fields = [
                curled[c * height : (c + 1) * height, ri * width : (ri + 1) * width]
                for c in range(3)
            ]
            work[0, ri, z] = deep * (across * fields[0] + along * fields[1]) - planar * fields[2]
            work[1, ri, z] = size * (across * fields[1] - along * fields[0])
        for comp in range(2):
            for ri in range(2):
                image[place.layer, comp, ri, half * place.core + z] = work[
                    comp, ri, z, pl.ds(rows * place.slab, rows), :
                ]

        for i in range(1, slabs):
            slab, device = place.slab_peer(i)
            send(
                work.at[:, :, pl.ds(z, 1), pl.ds(rows * slab, rows), :],
                image.at[place.layer, :, :, pl.ds(half * place.core + z, 1), :, :],
                sems.at[6, z], sems.at[7, z], device,
            )

    @pl.loop(0, chunks)
    def _(k):
        await_bytes(
            work.at[:, :, pl.ds(0, 1), pl.ds(0, rows * (slabs - 1)), :], sems.at[7, k]
        )
        gram(
            first_acc, gram_rows(bands, True), True, block, image, 2, lambda t: half * t + k,
        )

    first_sums = total(place, first_mine, first_slab, first_band, tail.at[0], lane_sums(first_tile, first_acc))
    pieces = lambda values, row: [
        values[row : row + 1, at : at + width] for at in range(0, values.shape[1], width)
    ]
    system = solve(
        scatter(pieces(first_sums, 0), solve_sources, solve_spread, solve_gather), 2 * bands, width
    )
    for row in range(2 * bands):
        for j in range(bands):
            mixing[row, j] = jnp.broadcast_to(
                system[row : row + 1, 2 * bands + j : 2 * bands + j + 1], (8, width)
            )

    @pl.loop(0, chunks)
    def _(k):
        slab_bytes = work.at[:, :, pl.ds(0, 1), pl.ds(0, rows * (slabs - 1)), :]
        plane_bytes = in_z.at[:, :, pl.ds(0, share * (2 * groups - 1)), :]
        await_bytes(slab_bytes, sems.at[0, k])
        await_bytes(plane_bytes, sems.at[2, k])
        await_bytes(plane_bytes, sems.at[4, k])
        await_bytes(slab_bytes, sems.at[6, k])

    for part in range(parts):
        await_bytes(eta.at[pl.ds(0, thin * 8 * (slabs - 1)), :], tail.at[2, part])

    quarter = width // groups
    second_acc[...] = jnp.zeros_like(second_acc)
    field_acc[...] = jnp.zeros_like(field_acc)
    lane = lax.broadcasted_iota(jnp.int32, (1, width), 1) // quarter
    deep_step = 8 if depth % 8 == 0 else 1

    def send_quarter(k):
        part, c = k // 3, k % 3
        for i in range(1, groups):
            group, device = place.band_peer(i)
            send(
                out_x.at[part * groups + group, c],
                in_z.at[c, :, pl.ds((part * length + depth * place.group) * 8, depth * 8), :],
                ends.at[0, k], ends.at[1, k], device,
            )

    @pl.loop(0, parts)
    def _(part):
        band_rows = pl.ds(part * 8, 8)
        across, along, planar = (
            waves[i, pl.ds(rows * place.slab + part * 8, 8), :] for i in range(3)
        )

        @pl.loop(0, depth)
        def _(z):
            tile_at = (z, band_rows, slice(None))
            deep = depths[z]
            scale = 1.0 / (planar * planar + deep * deep + 1.0)
            for comp in range(2):
                reals = [block[(i, comp, 0) + tile_at] for i in range(bands)]
                imags = [block[(i, comp, 1) + tile_at] for i in range(bands)]
                for j in range(bands):
                    real = image[(j, comp, 0) + tile_at]
                    imag = image[(j, comp, 1) + tile_at]
                    for i in range(bands):
                        real = real - (reals[i] * mixing[i, j] - imags[i] * mixing[bands + i, j])
                        imag = imag - (reals[i] * mixing[bands + i, j] + imags[i] * mixing[i, j])
                    search[(j, comp, 0) + tile_at] = real * scale
                    search[(j, comp, 1) + tile_at] = imag * scale

        @pl.loop(0, depth // deep_step)
        def _(group):
            planes = pl.ds(group * deep_step, deep_step)
            deep = depths[planes]
            size = jnp.sqrt(planar * planar + deep * deep)
            count = deep_step * 8
            lines = []
            for i in range(bands):
                fields = []
                for ri in range(2):
                    one = search[i, 0, ri, planes, band_rows, :]
                    two = search[i, 1, ri, planes, band_rows, :] * size
                    upright = one * deep
                    fields.append(
                        [
                            value.reshape(count, width)
                            for value in (
                                across * upright - along * two,
                                along * upright + across * two,
                                -planar * one,
                            )
                        ]
                    )
                curled = jnp.concatenate(
                    [jnp.concatenate([fields[0][c], fields[1][c]], 1) for c in range(3)], 0
                )
                lines.append(right_transform(curled, x_split.at[i]))
            at = pl.ds(group * count, count)
            for target in range(groups):
                for ri in range(2):
                    columns = slice(ri * width, (ri + 1) * width)
                    packed = lines[(-target) % groups][:, columns]
                    for spot in range(1, groups):
                        packed = jnp.where(
                            lane == spot, lines[(spot - target) % groups][:, columns], packed
                        )
                    for c in range(3):
                        out_x[part * groups + target, c, ri, at, :] = packed[c * count : (c + 1) * count]

        for c in range(3):
            for ri in range(2):
                in_z[c, ri, pl.ds((part * length + depth * place.group) * 8, depth * 8), :] = out_x[
                    part * groups + place.group, c, ri
                ]

        @pl.when(part == 0)
        def _():
            send_quarter(0)

    @pl.loop(0, 3 * parts)
    def _(k):
        part, c = k // 3, k % 3
        await_bytes(in_z.at[c, :, pl.ds(0, depth * 8 * (groups - 1)), :], ends.at[1, k])

        @pl.when(k == 0)
        def _():
            send_quarter(1)

        @pl.when(k + 2 < 3 * parts)
        def _():
            send_quarter(k + 2)

        base = part * length * 8

        @pl.loop(0, 4)
        def _(pair):
            first = base + 2 * pair
            keep_columns(out_z, c, first, left_transform(z_plus, columns_of(in_z, c, first)))

        for i in range(1, slabs):
            slab, device = place.slab_peer(i)
            send(
                out_z.at[c, :, pl.ds(base + thin * 8 * slab, thin * 8), :],
                in_y.at[place.slab, c, :, pl.ds(part * thin * 8, thin * 8), :],
                ends.at[2, k], ends.at[3, k], device,
            )
        for ri in range(2):
            in_y[place.slab, c, ri, pl.ds(part * thin * 8, thin * 8), :] = out_z[
                c, ri, pl.ds(base + thin * 8 * place.slab, thin * 8), :
            ]

    @pl.loop(0, thin)
    def _(z):
        for cell in range(2 * groups):
            for part in range(parts):
                values = cells[cell, pl.ds((part * thin + z) * 8, 8), :]
                values = pltpu.roll(values, lax.rem(width - quarter * place.group, width), 1)
                values = jnp.where(lane == 0, values, 0.0)
                reach = quarter
                while reach < width:
                    values = values + pltpu.roll(values, reach, 1)
                    reach *= 2
                local_eta[z, cell * share + part * 8 : cell * share + part * 8 + 8, :] = values

    base = gram(second_acc, 0, False, block, search, depth, lambda t: t)
    base = gram(second_acc, base, True, search, search, depth, lambda t: t)
    gram(second_acc, base, False, search, image, depth, lambda t: t)

    for c in range(3):
        for part in range(parts):
            await_bytes(
                in_y.at[pl.ds(0, slabs - 1), c, :, pl.ds(0, thin * 8), :],
                ends.at[3, part * 3 + c],
            )

        @pl.loop(0, thin)
        def _(z, c=c):
            stacked = jnp.concatenate(
                [
                    in_y[slab, c, ri, pl.ds(part * thin * 8 + 8 * z, 8), :]
                    for ri in range(2)
                    for slab in range(slabs)
                    for part in range(parts)
                ],
                0,
            )
            field = left_transform(y_plus, stacked)
            real, imag = field[:height], field[height:]
            weight = local_eta[z]
            real_weighted, imag_weighted = real * weight, imag * weight
            for shift in range(bands // 2 + 1):
                if shift == 0:
                    real_other, imag_other = real, imag
                else:
                    real_other = pltpu.roll(real, quarter * shift, 1)
                    imag_other = pltpu.roll(imag, quarter * shift, 1)
                real_term = real_weighted * real_other + imag_weighted * imag_other
                imag_term = real_weighted * imag_other - imag_weighted * real_other
                for place_of, term in ((2 * shift, real_term), (2 * shift + 1, imag_term)):
                    field_acc[place_of] += jnp.sum(term.reshape(height // 8, 8, width), axis=0)

    fields = jnp.sum(field_acc[...], axis=1)
    fields = pltpu.roll(fields, lax.rem(width - quarter * place.group, width), 1)
    values = lane_sums(second_tile, second_acc)
    if values.shape[1] > width:
        empty = jnp.zeros((fields.shape[0], values.shape[1] - width), jnp.float32)
        fields = jnp.concatenate([fields, empty], 1)
    second_sums = total(
        place, second_mine, second_slab, second_band, tail.at[1],
        jnp.concatenate([values, fields], 0),
    )
    listed = pieces(first_sums, 0) + pieces(second_sums, 0)
    for row in range(2 * (bands // 2 + 1)):
        listed.append(second_sums[8 + row : 9 + row, :width])
    results[...] = scatter(listed, result_sources, result_spread, result_gather) / cell_count

    @pl.loop(0, 3 * parts)
    def _(k):
        await_bytes(in_z.at[0, :, pl.ds(0, depth * 8 * (groups - 1)), :], ends.at[0, k])
        await_bytes(in_y.at[pl.ds(0, slabs - 1), 0, :, pl.ds(0, thin * 8), :], ends.at[2, k])


def vmem(count):
    return [pl.BlockSpec(memory_space=pltpu.VMEM)] * count


def round_up(value, step):
    return -(-value // step) * step


def step(block, materials, permittivity, bloch, groups, slabs):
    bands, _, _, depth, rows, width = block.shape
    half, height, length = depth // 2, rows * slabs, depth * groups
    share = height // (2 * groups)
    thin, parts, quarter = length // slabs, rows // 8, width // groups
    chunks = half
    first_count = 2 * gram_rows(bands, True)
    first_lanes = round_up(first_count, width)
    second_count = 2 * gram_rows(bands, False) + gram_rows(bands, True)
    second_lanes = round_up(second_count, width)
    field_rows = round_up(2 * (bands // 2 + 1), 8)
    message = (8 + field_rows, second_lanes)

    plain = dft_matrix(width, 1.0).T
    orders = []
    for band in range(bands):
        spots = np.arange(width) // quarter
        source = ((spots - band) % groups) * quarter + np.arange(width) % quarter
        orders.append(right_table(plain[:, np.concatenate([source, width + source])]))
    first_pieces, second_pieces = first_lanes // width, second_lanes // width
    solve_sources, *solve_tables = scatter_tables(system_entries(bands), first_pieces, width)
    result_sources, *result_tables = scatter_tables(
        result_entries(bands, width, first_pieces, second_pieces),
        first_pieces + second_pieces + 2 * (bands // 2 + 1),
        width,
    )
    tables = [
        np.stack(orders),
        right_table(dft_matrix(width, -1.0).T),
        left_table(height, 1.0),
        left_table(height, -1.0),
        *([] if length == height else [left_table(length, 1.0), left_table(length, -1.0)]),
        *solve_tables,
        *result_tables,
    ]
    single = lambda *shape: pltpu.VMEM(shape, jnp.float32)
    by_cell = (2 * groups, 3, 2, half * share, width)
    by_part = (parts * groups, 3, 2, depth * 8, width)
    out_x = [] if by_cell == by_part else [single(*by_part)]
    kernel = partial(
        step_kernel, groups, slabs, 2 + len(tables), solve_sources, result_sources
    )

    def body(*refs):
        refs = list(refs)
        if not out_x:
            outgoing = 2 + 2 * (2 + len(tables)) + 2 + 2
            refs.insert(outgoing + 4, refs[outgoing])
        kernel(*refs)

    return pl.pallas_call(
        body,
        in_specs=[pl.BlockSpec(memory_space=pltpu.SMEM)] * 2 + [pl.BlockSpec(memory_space=pl.ANY)] * (2 + len(tables)),
        out_specs=vmem(2),
        out_shape=[
            pltpu.VMEM(block.shape, jnp.float32),
            jax.ShapeDtypeStruct((result_tables[0].shape[0], width), jnp.float32),
        ],
        scratch_shapes=[
            *[pltpu.VMEM(array.shape, array.dtype) for array in (block, materials, *tables)],
            single(2, 2, half, height, width),
            single(*block.shape),
            single(*by_cell),
            single(3, 2, length * share, width),
            single(3, 2, length * share, width),
            single(*by_cell),
            *out_x,
            single(length * share, width),
            single(thin, height, width),
            single(2 * groups, thin * share, width),
            single(3, height, width),
            single(depth, 8, width),
            single(2 * bands, bands, 8, width),
            single(first_count, 8, width),
            single(first_lanes, width),
            single(2, 8, first_lanes),
            single(slabs, 8, first_lanes),
            single(groups, 8, first_lanes),
            single(second_count, 8, width),
            single(field_rows, 8, width),
            single(second_lanes, width),
            single(2, *message),
            single(slabs, *message),
            single(groups, *message),
            pltpu.SemaphoreType.DMA((8, chunks)),
            pltpu.SemaphoreType.DMA((parts, chunks)),
            pltpu.SemaphoreType.DMA((4, 3 * parts)),
            pltpu.SemaphoreType.DMA((4, 4)),
            pltpu.SemaphoreType.DMA((2 + len(tables),)),
        ],
        compiler_params=pltpu.CompilerParams(
            collective_id=0, has_side_effects=True, vmem_limit_bytes=VMEM_LIMIT
        ),
    )(permittivity, bloch, block, materials, *[jnp.asarray(table) for table in tables])


def shards(band_block, material_grid, inverse_permittivity, bloch_index):
    groups, slabs = lax.axis_size("band"), lax.axis_size("slab")
    size = 2 * band_block.shape[0]
    search_block, results = step(
        band_block, material_grid, inverse_permittivity, bloch_index, groups, slabs
    )
    results = results[:, :size].reshape(2, 2, size, size)
    return (search_block, results[0], results[1])


def solution(mesh):
    return jax.shard_map(
        shards,
        mesh=mesh,
        in_specs=(P(None, None, None, "band", "slab", None), P("slab", None, None), P(), P()),
        out_specs=(P(None, None, None, "band", "slab", None), P(), P()),
        check_vma=False,
    )
```

```python
from functools import partial
import math

import jax
import jax.numpy as jnp
import numpy as np
from jax import lax
from jax.experimental import pallas as pl
from jax.experimental.pallas import tpu as pltpu
from jax.sharding import PartitionSpec as P

KPOINTS = 8
HIGHEST = lax.Precision.HIGHEST
MESH = pl.DeviceIdType.MESH
VMEM_LIMIT = 54 * 1024 * 1024
WINDOW = 3


def halves(values):
    high = values.astype(jnp.bfloat16)
    return high, (values - high.astype(jnp.float32)).astype(jnp.bfloat16)


def dft_matrix(length, direction):
    indices = np.arange(length)
    angles = 2.0 * np.pi / length * (np.outer(indices, indices) % length)
    cosine, sine = np.cos(angles), direction * np.sin(angles)
    return np.block([[cosine, -sine], [sine, cosine]])


def numpy_halves(matrix):
    single = matrix.astype(np.float32)
    high = single.astype(jnp.bfloat16)
    low = (single - high.astype(np.float32)).astype(jnp.bfloat16)
    return high, low


def left_table(length, direction):
    return np.concatenate(numpy_halves(dft_matrix(length, direction)), 0)


def right_table(matrix):
    return np.concatenate(numpy_halves(matrix), 0)


def dot(left, right):
    return jnp.dot(left, right, preferred_element_type=jnp.float32)


def left_transform(table, values):
    size = values.shape[0]
    high, low = halves(values)
    main = dot(table[...], high)
    rest = dot(table[:size, :], low)
    return main[:size] + (main[size:] + rest)


def right_transform(values, table):
    size = values.shape[1]
    high, low = halves(values)
    return dot(jnp.concatenate([high, high], 1), table[...]) + dot(low, table[:size, :])


def gram(acc, base, hermitian, left, right, count, depth_of):
    bands, rows, lanes = left.shape[0], left.shape[4], left.shape[5]
    for i in range(bands):
        others = list(range(i if hermitian else 0, bands))

        def body(step, sums, i=i, others=others):
            depth = depth_of(step)
            sums = list(sums)
            for row in range(0, rows, 8):
                tile = (depth, pl.ds(row, 8), slice(None))
                for comp in range(2):
                    left_real = left[(i, comp, 0) + tile]
                    left_imag = left[(i, comp, 1) + tile]
                    for place, j in enumerate(others):
                        right_real = right[(j, comp, 0) + tile]
                        right_imag = right[(j, comp, 1) + tile]
                        sums[2 * place] += left_real * right_real + left_imag * right_imag
                        sums[2 * place + 1] += left_real * right_imag - left_imag * right_real
            return tuple(sums)

        zeros = tuple(jnp.zeros((8, lanes), jnp.float32) for _ in range(2 * len(others)))
        sums = lax.fori_loop(0, count, body, zeros)
        for place, value in enumerate(sums):
            acc[base + place] += value
        base += 2 * len(others)
    return base


def gram_rows(bands, hermitian):
    return bands * (bands + 1) if hermitian else 2 * bands * bands


def scatter_tables(entries, pieces, width):
    slots = {}
    rows = 8 * (-(-(1 + max(entry[2] for entry in entries)) // 8))
    for source, lane, row, column, sign in entries:
        columns = slots.setdefault((source, lane), {})
        columns.setdefault(column, {})[row] = sign
    blocks = []
    for source in range(pieces):
        depth = max([len(v) for (s, _), v in slots.items() if s == source], default=0)
        blocks += [(source, place) for place in range(depth)]
    spread = np.zeros((rows, width * len(blocks)), np.float32)
    gather = np.zeros((width * len(blocks), width), np.float32)
    for index, (source, place) in enumerate(blocks):
        for lane in range(width):
            columns = list(slots.get((source, lane), {}).items())
            if place < len(columns):
                column, signs = columns[place]
                gather[index * width + lane, column] = 1.0
                for row, sign in signs.items():
                    spread[row, index * width + lane] = sign
    return [source for source, _ in blocks], spread, gather.astype(jnp.bfloat16)


def scatter(values, sources, spread, gather):
    rows, width = spread.shape[0], values[0].shape[1]
    spots = jnp.concatenate(
        [
            jnp.broadcast_to(values[source], (rows, width))
            * spread[:, place * width : (place + 1) * width]
            for place, source in enumerate(sources)
        ],
        1,
    )
    high, rest = halves(spots)
    low = (spots - high.astype(jnp.float32)) - rest.astype(jnp.float32)
    return (dot(high, gather[...]) + dot(rest, gather[...])) + dot(
        low.astype(jnp.bfloat16), gather[...]
    )


def pair_list(bands, hermitian):
    return [(i, j) for i in range(bands) for j in range(i if hermitian else 0, bands)]


def complex_entries(source, base, pairs, put):
    entries = []
    for place, (i, j) in enumerate(pairs):
        for real_row, imag_row, column, sign in put(i, j):
            lane = base + 2 * place
            entries.append((source + lane // 128, lane % 128, real_row, column, 1.0))
            entries.append((source + (lane + 1) // 128, (lane + 1) % 128, imag_row, column, sign))
    return entries


def mirrored(i, j, put):
    return [put(i, j, 1.0)] if i == j else [put(i, j, 1.0), put(j, i, -1.0)]


def system_entries(bands):
    pairs = pair_list(bands, True)
    entries = []
    for offset in (0, bands):
        def left(i, j, sign):
            if offset == 0:
                return (i, bands + i, j, sign)
            return (bands + i, i, bands + j, -sign)

        entries += complex_entries(0, 0, pairs, lambda i, j: mirrored(i, j, left))
    return entries


def side_entries(bands):
    right = lambda i, j, sign: (i, bands + i, j, sign)
    return complex_entries(0, 0, pair_list(bands, True), lambda i, j: mirrored(i, j, right))


def result_entries(bands, width, first_pieces, second_pieces):
    size, own = 2 * bands, pair_list(bands, True)
    every = pair_list(bands, False)

    def spot(matrix, row, column):
        return lambda i, j, sign: (
            2 * size * matrix + row + i, 2 * size * matrix + size + row + i, column + j, sign
        )

    entries = complex_entries(0, 0, own, lambda i, j: mirrored(i, j, spot(0, 0, 0)))
    entries += complex_entries(
        first_pieces, 0, own, lambda i, j: mirrored(i, j, spot(1, 0, 0))
    )
    source, base = 2 * first_pieces, 0
    entries += complex_entries(
        source, base, every,
        lambda i, j: [spot(0, 0, bands)(i, j, 1.0), spot(0, bands, 0)(j, i, -1.0)],
    )
    base += gram_rows(bands, False)
    entries += complex_entries(
        source, base, own, lambda i, j: mirrored(i, j, spot(0, bands, bands))
    )
    base += gram_rows(bands, True)
    entries += complex_entries(
        source, base, every,
        lambda i, j: [spot(1, bands, 0)(i, j, 1.0), spot(1, 0, bands)(j, i, -1.0)],
    )
    source, known, entries = 0, entries, []
    for shift in range(bands // 2 + 1):
        for lane in range(width):
            i = lane // (width // bands)
            j = (i - shift) % bands
            places = [(i, j, 1.0)]
            if shift and 2 * shift != bands:
                places.append((j, i, -1.0))
            for row, column, sign in places:
                real_row, imag_row, at, sign = spot(1, bands, bands)(row, column, sign)
                entries.append((source + 2 * shift, lane, real_row, at, 1.0))
                if shift:
                    entries.append((source + 2 * shift + 1, lane, imag_row, at, sign))
    return known, entries


def solve(system, size, width):
    row_at = lax.broadcasted_iota(jnp.int32, system.shape, 0)
    for k in range(size):
        pivot = system[k : k + 1, :] / system[k : k + 1, k : k + 1]
        system = jnp.where(row_at == k, pivot, system - system[:, k : k + 1] * pivot)
    return system


def wave(length, weight, fraction, indices):
    signed = jnp.where(indices >= length // 2, indices - length, indices).astype(jnp.float32)
    return 2.0 * math.pi / length * (signed + weight * fraction)


class Place:
    def __init__(self, groups, slabs):
        self.groups, self.slabs = groups, slabs
        self.group = lax.axis_index("band")
        self.slab = lax.axis_index("slab")
        self.layer, self.core = self.slab // 2, self.slab % 2
        self.cell = 2 * self.group + self.core

    def slab_peer(self, step):
        slab = lax.rem(self.slab + step, self.slabs)
        return slab, (self.group, slab)

    def band_peer(self, step):
        group = lax.rem(self.group + step, self.groups)
        return group, (group, self.slab)

    def plane_peer(self, step):
        cell = lax.rem(self.cell + step, 2 * self.groups)
        return cell, (cell // 2, 2 * self.layer + cell % 2)


def enter(devices):
    barrier = pltpu.get_barrier_semaphore()
    for device in devices:
        pl.semaphore_signal(barrier, inc=1, device_id=device, device_id_type=MESH)
    pl.semaphore_wait(barrier, len(devices))


def send(source, target, send_sem, recv_sem, device):
    pltpu.make_async_remote_copy(
        src_ref=source,
        dst_ref=target,
        send_sem=send_sem,
        recv_sem=recv_sem,
        device_id=device,
        device_id_type=MESH,
    ).start()


def await_bytes(ref, sem):
    pltpu.make_async_copy(ref, ref, sem).wait()


def total_start(place, mine, first, sems, values):
    mine[0] = values
    first[place.slab] = values
    for step in range(1, place.slabs):
        _, device = place.slab_peer(step)
        send(mine.at[0], first.at[place.slab], sems.at[0], sems.at[1], device)


def total_turn(place, mine, first, second, sems):
    await_bytes(first.at[pl.ds(0, place.slabs - 1)], sems.at[1])
    values = first[0]
    for slab in range(1, place.slabs):
        values = values + first[slab]
    mine[1] = values
    second[place.group] = values
    for step in range(1, place.groups):
        _, device = place.band_peer(step)
        send(mine.at[1], second.at[place.group], sems.at[2], sems.at[3], device)


def total_end(place, first, second, sems):
    await_bytes(second.at[pl.ds(0, place.groups - 1)], sems.at[3])
    values = second[0]
    for group in range(1, place.groups):
        values = values + second[group]
    await_bytes(first.at[pl.ds(0, place.slabs - 1)], sems.at[0])
    await_bytes(second.at[pl.ds(0, place.groups - 1)], sems.at[2])
    return values


def lane_sums(tile, acc):
    rows = acc.shape[0]
    tile[...] = jnp.zeros_like(tile)
    tile[:rows, :] = jnp.sum(acc[...], axis=1)
    ones = jnp.ones((8, tile.shape[1]), jnp.float32)
    return lax.dot_general(
        ones, tile[...], (((1,), (1,)), ((), ())), precision=HIGHEST,
        preferred_element_type=jnp.float32,
    )


def step_kernel(
    groups, slabs, arrays, all_sources,
    permittivity, bloch, given, *refs,
):
    outside, refs = (given, *refs[: arrays - 1]), refs[arrays - 1 :]
    (search, results), inside, refs = refs[:2], refs[2 : arrays + 2], refs[arrays + 2 :]
    block, materials, x_split, x_minus, y_plus, y_minus = inside[:6]
    z_plus, z_minus = inside[6:8] if arrays == 16 else (y_plus, y_minus)
    (
        solve_spread, solve_gather, side_spread, side_gather,
        known_spread, known_gather, field_spread, field_gather,
    ) = inside[-8:]
    solve_sources, side_sources, known_sources, field_sources = all_sources
    (
        work, image, out_y, in_z, out_z, in_y, out_x, eta, local_eta, cells, waves, depths, mixing,
        own_acc, cross_acc, first_tile, own_mine, own_slab, own_band,
        cross_mine, cross_slab, cross_band,
        second_acc, field_acc, second_tile, second_mine, second_slab, second_band,
        field_mine, field_slab, field_band, inverse,
        sems, comes, ends, tail, paths, loads,
    ) = refs
    place = Place(groups, slabs)
    bands, _, _, depth, rows, width = block.shape
    half = depth // 2
    height = rows * slabs
    length = depth * groups
    share = out_y.shape[3] // half
    cell_count = length * height * width
    thin = length // slabs
    chunks = half
    parts = share // 8
    lead = min(WINDOW, chunks)

    for place_of, (source, target) in enumerate(zip(outside, inside)):
        pltpu.make_async_copy(source, target, loads.at[place_of]).start()

    enter(
        [place.slab_peer(i)[1] for i in range(1, slabs)]
        + [
            (lax.rem(place.group + i, groups), 2 * place.layer + core)
            for i in range(1, groups)
            for core in range(2)
        ]
    )

    def send_out(k):
        for i in range(1, slabs):
            slab, device = place.slab_peer(i)
            send(
                given.at[slab // 2, :, :, pl.ds(half * (slab % 2) + k, 1), :, :],
                work.at[:, :, pl.ds(k, 1), pl.ds(rows * place.slab, rows), :],
                sems.at[0, k], sems.at[1, k], device,
            )

    @pl.loop(0, lead)
    def _(k):
        send_out(k)

    for place_of, (source, target) in enumerate(zip(outside, inside)):
        pltpu.make_async_copy(source, target, loads.at[place_of]).wait()

    @pl.loop(0, thin)
    def _(z):
        for cell in range(2 * groups):
            for part in range(parts):
                found = materials[z, pl.ds(cell * share + part * 8, 8), :]
                values = jnp.zeros(found.shape, jnp.float32)
                for material in range(permittivity.shape[0]):
                    values = jnp.where(found == material, permittivity[material] / cell_count, values)
                cells[cell, pl.ds((part * thin + z) * 8, 8), :] = values

    reach = slabs // 4
    first_layer = reach * (place.layer // reach)
    mirror = slabs // 2 - 1 - place.layer

    def near_peer(step):
        layer = first_layer + lax.rem(place.layer - first_layer + step, reach)
        return layer

    def cell_rows(part, slab):
        return pl.ds((part * length + thin * slab) * 8, thin * 8)

    def send_cells(part, layer, core, send_sem, recv_sem):
        send(
            cells.at[2 * place.group + core, pl.ds(part * thin * 8, thin * 8), :],
            eta.at[cell_rows(part, place.slab), :],
            send_sem, recv_sem, (place.group, 2 * layer + core),
        )

    def send_near(part):
        for i in range(1, reach):
            for core in range(2):
                send_cells(part, near_peer(i), core, paths.at[0, part], paths.at[1, part])
        send_cells(part, place.layer, 1 - place.core, paths.at[0, part], paths.at[1, part])

    def hand_on(part):
        await_bytes(eta.at[pl.ds(0, 2 * thin * 8), :], paths.at[3, part])
        for i in range(1, reach):
            for core in range(2):
                at = cell_rows(part, 2 * mirror + core)
                send(
                    eta.at[at, :], eta.at[at, :], paths.at[4, part], paths.at[5, part],
                    (place.group, 2 * near_peer(i) + place.core),
                )

    for part in range(parts):
        target = pl.ds((part * length + thin * place.slab) * 8, thin * 8)
        eta[target, :] = cells[place.cell, pl.ds(part * thin * 8, thin * 8), :]

    fraction = (bloch[0].astype(jnp.float32) + 1.0) / KPOINTS
    at_x = lax.broadcasted_iota(jnp.int32, (height, width), 1)
    at_y = lax.broadcasted_iota(jnp.int32, (height, width), 0)
    wave_x, wave_y = wave(width, 0.5, fraction, at_x), wave(height, 0.35, fraction, at_y)
    planar = jnp.sqrt(wave_x * wave_x + wave_y * wave_y)
    waves[0], waves[1], waves[2] = wave_x / planar, wave_y / planar, planar

    @pl.loop(0, depth)
    def _(z):
        at_z = jnp.broadcast_to(place.group * depth + z, (8, width))
        depths[z] = wave(length, 0.2, fraction, at_z)

    own_acc[...] = jnp.zeros_like(own_acc)
    cross_acc[...] = jnp.zeros_like(cross_acc)
    gram(own_acc, 0, True, block, block, depth, lambda t: t)
    total_start(place, own_mine, own_slab, tail.at[0], lane_sums(first_tile, own_acc))

    @pl.loop(0, chunks)
    def _(z):
        await_bytes(
            work.at[:, :, pl.ds(0, 1), pl.ds(0, rows * (slabs - 1)), :], sems.at[1, z]
        )

        @pl.when(z + lead < chunks)
        def _():
            send_out(z + lead)

        for part in range(parts):

            @pl.when(z == 1 + 4 * part)
            def _(part=part):
                send_near(part)

        @pl.when(z == chunks - 1)
        def _():
            for part in range(parts):
                for core in range(2):
                    send_cells(part, mirror, core, paths.at[2, part], paths.at[3, part])

        for comp in range(2):
            for ri in range(2):
                work[comp, ri, z, pl.ds(rows * place.slab, rows), :] = block[
                    place.layer, comp, ri, half * place.core + z
                ]
        across, along, planar = waves[0], waves[1], waves[2]
        deep = depths[half * place.core + z, 0:1, :]
        size = jnp.sqrt(planar * planar + deep * deep)
        fields = []
        for ri in range(2):
            one = work[0, ri, z]
            two = work[1, ri, z] * size
            upright = one * deep
            fields.append(
                [across * upright - along * two, along * upright + across * two, -planar * one]
            )
        curled = jnp.concatenate(
            [jnp.concatenate([fields[0][c], fields[1][c]], 1) for c in range(3)], 0
        )
        lines = right_transform(curled, x_split.at[0])
        stacked = jnp.concatenate(
            [
                jnp.concatenate(
                    [
                        lines[c * height : (c + 1) * height, :width],
                        lines[c * height : (c + 1) * height, width:],
                    ],
                    0,
                )
                for c in range(3)
            ],
            1,
        )
        planes = left_transform(y_plus, stacked)
        for c in range(3):
            for ri in range(2):
                for cell in range(2 * groups):
                    for part in range(parts):
                        base = ri * height + cell * share + part * 8
                        out_y[cell, c, ri, pl.ds((part * half + z) * 8, 8), :] = planes[
                            base : base + 8, c * width : (c + 1) * width
                        ]

        for part in range(parts):
            source = pl.ds((part * half + z) * 8, 8)
            target = pl.ds((part * length + place.cell * half + z) * 8, 8)
            for i in range(1, 2 * groups):
                cell, device = place.plane_peer(i)
                send(
                    out_y.at[cell, :, :, source, :],
                    in_z.at[:, :, target, :],
                    sems.at[2, z], comes.at[part, z], device,
                )
            for c in range(3):
                for ri in range(2):
                    in_z[c, ri, target, :] = out_y[place.cell, c, ri, source, :]

    def columns_of(source, c, first):
        return jnp.concatenate(
            [
                jnp.concatenate(
                    [source[c, ri, pl.ds(first + j, length, stride=8), :] for ri in range(2)], 0
                )
                for j in range(2)
            ],
            1,
        )

    def keep_columns(target, c, first, values):
        for j in range(2):
            for ri in range(2):
                target[c, ri, pl.ds(first + j, length, stride=8), :] = values[
                    ri * length : (ri + 1) * length, j * width : (j + 1) * width
                ]

    hand_on(0)
    for part in range(parts):
        @pl.loop(0, chunks)
        def _(k, part=part):
            await_bytes(in_z.at[:, :, pl.ds(0, 8 * (2 * groups - 1)), :], comes.at[part, k])

        @pl.loop(0, 4)
        def _(pair, part=part):
            first = part * length * 8 + 2 * pair
            for c in range(3):
                keep_columns(in_z, c, first, left_transform(z_plus, columns_of(in_z, c, first)))

    for part in range(1, parts):
        hand_on(part)
    total_turn(place, own_mine, own_slab, own_band, tail.at[0])

    def send_back(k, part):
        for i in range(1, 2 * groups):
            cell, device = place.plane_peer(i)
            send(
                out_z.at[:, :, pl.ds((part * length + cell * half + k) * 8, 8), :],
                in_y.at[place.cell, :, :, pl.ds((part * half + k) * 8, 8), :],
                sems.at[4, k], sems.at[5, k], device,
            )

    for part in range(parts):
        await_bytes(eta.at[pl.ds(0, thin * 8 * (2 * reach - 1)), :], paths.at[1, part])
        if reach > 1:
            await_bytes(eta.at[pl.ds(0, thin * 16 * (reach - 1)), :], paths.at[5, part])

        @pl.loop(0, 4)
        def _(pair, part=part):
            first = part * length * 8 + 2 * pair
            weight = jnp.concatenate(
                [eta[pl.ds(first + j, length, stride=8), :] for j in range(2)], 1
            )
            weight = jnp.concatenate([weight, weight], 0)
            for c in range(3):
                field = columns_of(in_z, c, first) * weight
                keep_columns(out_z, c, first, left_transform(z_minus, field))

        send_back(0, part)

    @pl.loop(1, lead)
    def _(k):
        for part in range(parts):
            send_back(k, part)

    @pl.loop(0, chunks)
    def _(z):
        for c in range(3):
            for ri in range(2):
                for part in range(parts):
                    in_y[place.cell, c, ri, pl.ds((part * half + z) * 8, 8), :] = out_z[
                        c, ri, pl.ds((part * length + place.cell * half + z) * 8, 8), :
                    ]
        await_bytes(in_y.at[pl.ds(0, 2 * groups - 1), :, :, pl.ds(0, share), :], sems.at[5, z])

        @pl.when(z + lead < chunks)
        def _():
            for part in range(parts):
                send_back(z + lead, part)


        stacked = jnp.concatenate(
            [
                jnp.concatenate(
                    [
                        in_y[cell, c, ri, pl.ds((part * half + z) * 8, 8), :]
                        for ri in range(2)
                        for cell in range(2 * groups)
                        for part in range(parts)
                    ],
                    0,
                )
                for c in range(3)
            ],
            1,
        )
        planes = left_transform(y_minus, stacked)
        lines = jnp.concatenate(
            [
                jnp.concatenate(
                    [
                        planes[:height, c * width : (c + 1) * width],
                        planes[height:, c * width : (c + 1) * width],
                    ],
                    1,
                )
                for c in range(3)
            ],
            0,
        )
        curled = right_transform(lines, x_minus)
        across, along, planar = waves[0], waves[1], waves[2]
        deep = depths[half * place.core + z, 0:1, :]
        size = jnp.sqrt(planar * planar + deep * deep)
        for ri in range(2):
            fields = [
                curled[c * height : (c + 1) * height, ri * width : (ri + 1) * width]
                for c in range(3)
            ]
            work[0, ri, z] = deep * (across * fields[0] + along * fields[1]) - planar * fields[2]
            work[1, ri, z] = size * (across * fields[1] - along * fields[0])
        for comp in range(2):
            for ri in range(2):
                image[place.layer, comp, ri, half * place.core + z] = work[
                    comp, ri, z, pl.ds(rows * place.slab, rows), :
                ]

        for i in range(1, slabs):
            slab, device = place.slab_peer(i)
            send(
                work.at[:, :, pl.ds(z, 1), pl.ds(rows * slab, rows), :],
                image.at[place.layer, :, :, pl.ds(half * place.core + z, 1), :, :],
                sems.at[6, z], sems.at[7, z], device,
            )

    own_sums = total_end(place, own_slab, own_band, tail.at[0])
    pieces = lambda values, row: [
        values[row : row + 1, at : at + width] for at in range(0, values.shape[1], width)
    ]
    system = scatter(pieces(own_sums, 0), solve_sources, solve_spread, solve_gather)
    rows_at = lax.broadcasted_iota(jnp.int32, system.shape, 0)
    lanes_at = lax.broadcasted_iota(jnp.int32, system.shape, 1)
    inverse[...] = solve(
        jnp.where(lanes_at == rows_at + 2 * bands, 1.0, system), 2 * bands, width
    )

    @pl.loop(0, chunks)
    def _(k):
        await_bytes(
            work.at[:, :, pl.ds(0, 1), pl.ds(0, rows * (slabs - 1)), :], sems.at[7, k]
        )
        gram(
            cross_acc, 0, True, block, image, 2, lambda t: half * t + k,
        )

    total_start(place, cross_mine, cross_slab, tail.at[1], lane_sums(first_tile, cross_acc))
    total_turn(place, cross_mine, cross_slab, cross_band, tail.at[1])
    cross_sums = total_end(place, cross_slab, cross_band, tail.at[1])
    side = scatter(pieces(cross_sums, 0), side_sources, side_spread, side_gather)
    factors = inverse[...]
    system = factors[:, 2 * bands : 2 * bands + 1] * side[0:1, :]
    for k in range(1, 2 * bands):
        system += factors[:, 2 * bands + k : 2 * bands + k + 1] * side[k : k + 1, :]
    for row in range(2 * bands):
        for j in range(bands):
            mixing[row, j] = jnp.broadcast_to(
                system[row : row + 1, j : j + 1], (8, width)
            )

    @pl.loop(0, chunks)
    def _(k):
        slab_bytes = work.at[:, :, pl.ds(0, 1), pl.ds(0, rows * (slabs - 1)), :]
        plane_bytes = in_z.at[:, :, pl.ds(0, share * (2 * groups - 1)), :]
        await_bytes(slab_bytes, sems.at[0, k])
        await_bytes(plane_bytes, sems.at[2, k])
        await_bytes(plane_bytes, sems.at[4, k])
        await_bytes(slab_bytes, sems.at[6, k])

    for part in range(parts):
        await_bytes(eta.at[pl.ds(0, thin * 8 * (2 * reach - 1)), :], paths.at[0, part])
        await_bytes(eta.at[pl.ds(0, thin * 16), :], paths.at[2, part])
        if reach > 1:
            await_bytes(eta.at[pl.ds(0, thin * 16 * (reach - 1)), :], paths.at[4, part])

    quarter = width // groups
    second_acc[...] = jnp.zeros_like(second_acc)
    field_acc[...] = jnp.zeros_like(field_acc)
    lane = lax.broadcasted_iota(jnp.int32, (1, width), 1) // quarter
    deep_step = 8 if depth % 8 == 0 else 1

    def send_rows(k, first, count):
        part, c = k // 3, k % 3
        base = (part * length + depth * place.group) * 8
        for i in range(1, groups):
            group, device = place.band_peer(i)
            send(
                out_x.at[part * groups + group, c, :, pl.ds(first, count), :],
                in_z.at[c, :, pl.ds(base + first, count), :],
                ends.at[0, k], ends.at[1, k], device,
            )

    def send_quarter(k):
        send_rows(k, 0, depth * 8)

    @pl.loop(0, parts)
    def _(part):
        band_rows = pl.ds(part * 8, 8)
        across, along, planar = (
            waves[i, pl.ds(rows * place.slab + part * 8, 8), :] for i in range(3)
        )

        @pl.loop(0, depth // deep_step)
        def _(group):
            @pl.loop(group * deep_step, (group + 1) * deep_step)
            def _(z):
                tile_at = (z, band_rows, slice(None))
                deep = depths[z]
                scale = 1.0 / (planar * planar + deep * deep + 1.0)
                for comp in range(2):
                    reals = [block[(i, comp, 0) + tile_at] for i in range(bands)]
                    imags = [block[(i, comp, 1) + tile_at] for i in range(bands)]
                    for j in range(bands):
                        real = image[(j, comp, 0) + tile_at]
                        imag = image[(j, comp, 1) + tile_at]
                        for i in range(bands):
                            real = real - (reals[i] * mixing[i, j] - imags[i] * mixing[bands + i, j])
                            imag = imag - (reals[i] * mixing[bands + i, j] + imags[i] * mixing[i, j])
                        search[(j, comp, 0) + tile_at] = real * scale
                        search[(j, comp, 1) + tile_at] = imag * scale

            planes = pl.ds(group * deep_step, deep_step)
            deep = depths[planes]
            size = jnp.sqrt(planar * planar + deep * deep)
            count = deep_step * 8
            lines = []
            for i in range(bands):
                fields = []
                for ri in range(2):
                    one = search[i, 0, ri, planes, band_rows, :]
                    two = search[i, 1, ri, planes, band_rows, :] * size
                    upright = one * deep
                    fields.append(
                        [
                            value.reshape(count, width)
                            for value in (
                                across * upright - along * two,
                                along * upright + across * two,
                                -planar * one,
                            )
                        ]
                    )
                curled = jnp.concatenate(
                    [jnp.concatenate([fields[0][c], fields[1][c]], 1) for c in range(3)], 0
                )
                lines.append(right_transform(curled, x_split.at[i]))
            at = pl.ds(group * count, count)
            for target in range(groups):
                for ri in range(2):
                    columns = slice(ri * width, (ri + 1) * width)
                    packed = lines[(-target) % groups][:, columns]
                    for spot in range(1, groups):
                        packed = jnp.where(
                            lane == spot, lines[(spot - target) % groups][:, columns], packed
                        )
                    for c in range(3):
                        out_x[part * groups + target, c, ri, at, :] = packed[c * count : (c + 1) * count]

            @pl.when(part == 0)
            def _():
                send_rows(0, group * count, count)

        for c in range(3):
            for ri in range(2):
                in_z[c, ri, pl.ds((part * length + depth * place.group) * 8, depth * 8), :] = out_x[
                    part * groups + place.group, c, ri
                ]

    @pl.loop(0, 3 * parts)
    def _(k):
        part, c = k // 3, k % 3
        await_bytes(in_z.at[c, :, pl.ds(0, depth * 8 * (groups - 1)), :], ends.at[1, k])

        @pl.when(k == 0)
        def _():
            send_quarter(1)

        @pl.when(k + 2 < 3 * parts)
        def _():
            send_quarter(k + 2)

        base = part * length * 8

        @pl.loop(0, 4)
        def _(pair):
            first = base + 2 * pair
            keep_columns(out_z, c, first, left_transform(z_plus, columns_of(in_z, c, first)))

        for i in range(1, slabs):
            slab, device = place.slab_peer(i)
            send(
                out_z.at[c, :, pl.ds(base + thin * 8 * slab, thin * 8), :],
                in_y.at[place.slab, c, :, pl.ds(part * thin * 8, thin * 8), :],
                ends.at[2, k], ends.at[3, k], device,
            )
        for ri in range(2):
            in_y[place.slab, c, ri, pl.ds(part * thin * 8, thin * 8), :] = out_z[
                c, ri, pl.ds(base + thin * 8 * place.slab, thin * 8), :
            ]

    @pl.loop(0, thin)
    def _(z):
        for cell in range(2 * groups):
            for part in range(parts):
                values = cells[cell, pl.ds((part * thin + z) * 8, 8), :]
                values = pltpu.roll(values, lax.rem(width - quarter * place.group, width), 1)
                values = jnp.where(lane == 0, values, 0.0)
                reach = quarter
                while reach < width:
                    values = values + pltpu.roll(values, reach, 1)
                    reach *= 2
                local_eta[z, cell * share + part * 8 : cell * share + part * 8 + 8, :] = values

    base = gram(second_acc, 0, False, block, search, depth, lambda t: t)
    base = gram(second_acc, base, True, search, search, depth, lambda t: t)
    gram(second_acc, base, False, search, image, depth, lambda t: t)
    total_start(place, second_mine, second_slab, tail.at[2], lane_sums(second_tile, second_acc))

    def add_products(real, imag, weight):
        real_weighted, imag_weighted = real * weight, imag * weight
        for shift in range(bands // 2 + 1):
            if shift == 0:
                real_other, imag_other = real, imag
            else:
                real_other = pltpu.roll(real, quarter * shift, 1)
                imag_other = pltpu.roll(imag, quarter * shift, 1)
            real_term = real_weighted * real_other + imag_weighted * imag_other
            imag_term = real_weighted * imag_other - imag_weighted * real_other
            for place_of, term in ((2 * shift, real_term), (2 * shift + 1, imag_term)):
                field_acc[place_of] += jnp.sum(term.reshape(height // 8, 8, width), axis=0)

    for c in range(3):
        for part in range(parts):
            await_bytes(
                in_y.at[pl.ds(0, slabs - 1), c, :, pl.ds(0, thin * 8), :],
                ends.at[3, part * 3 + c],
            )

        @pl.loop(0, thin // 2)
        def _(pair, c=c):
            stacked = jnp.concatenate(
                [
                    jnp.concatenate(
                        [
                            in_y[slab, c, ri, pl.ds(part * thin * 8 + 16 * pair + 8 * j, 8), :]
                            for ri in range(2)
                            for slab in range(slabs)
                            for part in range(parts)
                        ],
                        0,
                    )
                    for j in range(2)
                ],
                1,
            )
            planes = left_transform(y_plus, stacked)
            for j in range(2):
                lanes = slice(j * width, (j + 1) * width)
                add_products(planes[:height, lanes], planes[height:, lanes], local_eta[2 * pair + j])

    fields = jnp.sum(field_acc[...], axis=1)
    fields = pltpu.roll(fields, lax.rem(width - quarter * place.group, width), 1)
    total_start(place, field_mine, field_slab, tail.at[3], fields)
    total_turn(place, second_mine, second_slab, second_band, tail.at[2])
    total_turn(place, field_mine, field_slab, field_band, tail.at[3])
    second_sums = total_end(place, second_slab, second_band, tail.at[2])
    listed = pieces(own_sums, 0) + pieces(cross_sums, 0) + pieces(second_sums, 0)
    known = scatter(listed, known_sources, known_spread, known_gather)
    fields = total_end(place, field_slab, field_band, tail.at[3])
    listed = [fields[row : row + 1] for row in range(2 * (bands // 2 + 1))]
    fields = scatter(listed, field_sources, field_spread, field_gather)
    results[...] = (known + fields) / cell_count

    @pl.loop(0, 3 * parts)
    def _(k):
        await_bytes(in_z.at[0, :, pl.ds(0, depth * 8 * (groups - 1)), :], ends.at[0, k])
        await_bytes(in_y.at[pl.ds(0, slabs - 1), 0, :, pl.ds(0, thin * 8), :], ends.at[2, k])


def vmem(count):
    return [pl.BlockSpec(memory_space=pltpu.VMEM)] * count


def round_up(value, step):
    return -(-value // step) * step


def step(block, materials, permittivity, bloch, groups, slabs):
    bands, _, _, depth, rows, width = block.shape
    half, height, length = depth // 2, rows * slabs, depth * groups
    share = height // (2 * groups)
    thin, parts, quarter = length // slabs, rows // 8, width // groups
    chunks = half
    first_count = gram_rows(bands, True)
    first_lanes = round_up(first_count, width)
    second_count = 2 * gram_rows(bands, False) + gram_rows(bands, True)
    second_lanes = round_up(second_count, width)
    field_rows = round_up(2 * (bands // 2 + 1), 8)

    plain = dft_matrix(width, 1.0).T
    orders = []
    for band in range(bands):
        spots = np.arange(width) // quarter
        source = ((spots - band) % groups) * quarter + np.arange(width) % quarter
        orders.append(right_table(plain[:, np.concatenate([source, width + source])]))
    first_pieces, second_pieces = first_lanes // width, second_lanes // width
    known, fields = result_entries(bands, width, first_pieces, second_pieces)
    scattered = [
        scatter_tables(entries, count, width)
        for entries, count in (
            (system_entries(bands), first_pieces),
            (side_entries(bands), first_pieces),
            (known, 2 * first_pieces + second_pieces),
            (fields, 2 * (bands // 2 + 1)),
        )
    ]
    tables = [
        np.stack(orders),
        right_table(dft_matrix(width, -1.0).T),
        left_table(height, 1.0),
        left_table(height, -1.0),
        *([] if length == height else [left_table(length, 1.0), left_table(length, -1.0)]),
        *[table for _, *pair in scattered for table in pair],
    ]
    single = lambda *shape: pltpu.VMEM(shape, jnp.float32)
    slots = lambda *tile: [single(2, *tile), single(slabs, *tile), single(groups, *tile)]
    by_cell = (2 * groups, 3, 2, half * share, width)
    by_part = (parts * groups, 3, 2, depth * 8, width)
    out_x = [] if by_cell == by_part else [single(*by_part)]
    kernel = partial(
        step_kernel, groups, slabs, 2 + len(tables), [sources for sources, *_ in scattered]
    )

    def body(*refs):
        refs = list(refs)
        if not out_x:
            outgoing = 2 + 2 * (2 + len(tables)) + 2 + 2
            refs.insert(outgoing + 4, refs[outgoing])
        kernel(*refs)

    return pl.pallas_call(
        body,
        in_specs=[pl.BlockSpec(memory_space=pltpu.SMEM)] * 2 + [pl.BlockSpec(memory_space=pl.ANY)] * (2 + len(tables)),
        out_specs=vmem(2),
        out_shape=[
            pltpu.VMEM(block.shape, jnp.float32),
            jax.ShapeDtypeStruct((8 * bands, width), jnp.float32),
        ],
        scratch_shapes=[
            *[pltpu.VMEM(array.shape, array.dtype) for array in (block, materials, *tables)],
            single(2, 2, half, height, width),
            single(*block.shape),
            single(*by_cell),
            single(3, 2, length * share, width),
            single(3, 2, length * share, width),
            single(*by_cell),
            *out_x,
            single(length * share, width),
            single(thin, height, width),
            single(2 * groups, thin * share, width),
            single(3, height, width),
            single(depth, 8, width),
            single(2 * bands, bands, 8, width),
            single(first_count, 8, width),
            single(first_count, 8, width),
            single(first_lanes, width),
            *slots(8, first_lanes),
            *slots(8, first_lanes),
            single(second_count, 8, width),
            single(field_rows, 8, width),
            single(second_lanes, width),
            *slots(8, second_lanes),
            *slots(field_rows, width),
            single(2 * bands, width),
            pltpu.SemaphoreType.DMA((8, chunks)),
            pltpu.SemaphoreType.DMA((parts, chunks)),
            pltpu.SemaphoreType.DMA((4, 3 * parts)),
            pltpu.SemaphoreType.DMA((4, 4)),
            pltpu.SemaphoreType.DMA((6, parts)),
            pltpu.SemaphoreType.DMA((2 + len(tables),)),
        ],
        compiler_params=pltpu.CompilerParams(
            collective_id=0, has_side_effects=True, vmem_limit_bytes=VMEM_LIMIT
        ),
    )(permittivity, bloch, block, materials, *[jnp.asarray(table) for table in tables])


def shards(band_block, material_grid, inverse_permittivity, bloch_index):
    groups, slabs = lax.axis_size("band"), lax.axis_size("slab")
    size = 2 * band_block.shape[0]
    search_block, results = step(
        band_block, material_grid, inverse_permittivity, bloch_index, groups, slabs
    )
    results = results[:, :size].reshape(2, 2, size, size)
    return (search_block, results[0], results[1])


def solution(mesh):
    return jax.shard_map(
        shards,
        mesh=mesh,
        in_specs=(P(None, None, None, "band", "slab", None), P("slab", None, None), P(), P()),
        out_specs=(P(None, None, None, "band", "slab", None), P(), P()),
        check_vma=False,
    )
```

```python
from functools import partial
import math

import jax
import jax.numpy as jnp
import numpy as np
from jax import lax
from jax.experimental import pallas as pl
from jax.experimental.pallas import tpu as pltpu
from jax.sharding import PartitionSpec as P

KPOINTS = 8
HIGHEST = lax.Precision.HIGHEST
MESH = pl.DeviceIdType.MESH
VMEM_LIMIT = 54 * 1024 * 1024
WINDOW = 2


def halves(values):
    high = values.astype(jnp.bfloat16)
    return high, (values - high.astype(jnp.float32)).astype(jnp.bfloat16)


def dft_matrix(length, direction):
    indices = np.arange(length)
    angles = 2.0 * np.pi / length * (np.outer(indices, indices) % length)
    cosine, sine = np.cos(angles), direction * np.sin(angles)
    return np.block([[cosine, -sine], [sine, cosine]])


def numpy_halves(matrix):
    single = matrix.astype(np.float32)
    high = single.astype(jnp.bfloat16)
    low = (single - high.astype(np.float32)).astype(jnp.bfloat16)
    return high, low


def left_table(length, direction):
    return np.concatenate(numpy_halves(dft_matrix(length, direction)), 0)


def right_table(matrix):
    return np.concatenate(numpy_halves(matrix), 0)


def dot(left, right):
    return jnp.dot(left, right, preferred_element_type=jnp.float32)


def left_transform(table, values):
    size = values.shape[0]
    high, low = halves(values)
    main = dot(table[...], high)
    rest = dot(table[:size, :], low)
    return main[:size] + (main[size:] + rest)


def right_transform(values, table):
    size = values.shape[1]
    high, low = halves(values)
    return dot(jnp.concatenate([high, high], 1), table[...]) + dot(low, table[:size, :])


def gram(acc, base, hermitian, left, right, count, depth_of):
    bands, rows, lanes = left.shape[0], left.shape[4], left.shape[5]
    for i in range(bands):
        others = list(range(i if hermitian else 0, bands))

        def body(step, sums, i=i, others=others):
            depth = depth_of(step)
            sums = list(sums)
            for row in range(0, rows, 8):
                tile = (depth, pl.ds(row, 8), slice(None))
                for comp in range(2):
                    left_real = left[(i, comp, 0) + tile]
                    left_imag = left[(i, comp, 1) + tile]
                    for place, j in enumerate(others):
                        right_real = right[(j, comp, 0) + tile]
                        right_imag = right[(j, comp, 1) + tile]
                        sums[2 * place] += left_real * right_real + left_imag * right_imag
                        sums[2 * place + 1] += left_real * right_imag - left_imag * right_real
            return tuple(sums)

        zeros = tuple(jnp.zeros((8, lanes), jnp.float32) for _ in range(2 * len(others)))
        sums = lax.fori_loop(0, count, body, zeros)
        for place, value in enumerate(sums):
            acc[base + place] += value
        base += 2 * len(others)
    return base


def gram_rows(bands, hermitian):
    return bands * (bands + 1) if hermitian else 2 * bands * bands


def scatter_tables(entries, pieces, width):
    slots = {}
    rows = 8 * (-(-(1 + max(entry[2] for entry in entries)) // 8))
    for source, lane, row, column, sign in entries:
        columns = slots.setdefault((source, lane), {})
        columns.setdefault(column, {})[row] = sign
    blocks = []
    for source in range(pieces):
        depth = max([len(v) for (s, _), v in slots.items() if s == source], default=0)
        blocks += [(source, place) for place in range(depth)]
    spread = np.zeros((rows, width * len(blocks)), np.float32)
    gather = np.zeros((width * len(blocks), width), np.float32)
    for index, (source, place) in enumerate(blocks):
        for lane in range(width):
            columns = list(slots.get((source, lane), {}).items())
            if place < len(columns):
                column, signs = columns[place]
                gather[index * width + lane, column] = 1.0
                for row, sign in signs.items():
                    spread[row, index * width + lane] = sign
    return [source for source, _ in blocks], spread, gather.astype(jnp.bfloat16)


def scatter(values, sources, spread, gather):
    rows, width = spread.shape[0], values[0].shape[1]
    spots = jnp.concatenate(
        [
            jnp.broadcast_to(values[source], (rows, width))
            * spread[:, place * width : (place + 1) * width]
            for place, source in enumerate(sources)
        ],
        1,
    )
    high, rest = halves(spots)
    low = (spots - high.astype(jnp.float32)) - rest.astype(jnp.float32)
    return (dot(high, gather[...]) + dot(rest, gather[...])) + dot(
        low.astype(jnp.bfloat16), gather[...]
    )


def pair_list(bands, hermitian):
    return [(i, j) for i in range(bands) for j in range(i if hermitian else 0, bands)]


def complex_entries(source, base, pairs, put):
    entries = []
    for place, (i, j) in enumerate(pairs):
        for real_row, imag_row, column, sign in put(i, j):
            lane = base + 2 * place
            entries.append((source + lane // 128, lane % 128, real_row, column, 1.0))
            entries.append((source + (lane + 1) // 128, (lane + 1) % 128, imag_row, column, sign))
    return entries


def mirrored(i, j, put):
    return [put(i, j, 1.0)] if i == j else [put(i, j, 1.0), put(j, i, -1.0)]


def system_entries(bands):
    pairs = pair_list(bands, True)
    entries = []
    for offset in (0, bands):
        def left(i, j, sign):
            if offset == 0:
                return (i, bands + i, j, sign)
            return (bands + i, i, bands + j, -sign)

        entries += complex_entries(0, 0, pairs, lambda i, j: mirrored(i, j, left))
    return entries


def side_entries(bands):
    right = lambda i, j, sign: (i, bands + i, j, sign)
    return complex_entries(0, 0, pair_list(bands, True), lambda i, j: mirrored(i, j, right))


def result_entries(bands, width, first_pieces, second_pieces):
    size, own = 2 * bands, pair_list(bands, True)
    every = pair_list(bands, False)

    def spot(matrix, row, column):
        return lambda i, j, sign: (
            2 * size * matrix + row + i, 2 * size * matrix + size + row + i, column + j, sign
        )

    entries = complex_entries(0, 0, own, lambda i, j: mirrored(i, j, spot(0, 0, 0)))
    entries += complex_entries(
        first_pieces, 0, own, lambda i, j: mirrored(i, j, spot(1, 0, 0))
    )
    source, base = 2 * first_pieces, 0
    entries += complex_entries(
        source, base, every,
        lambda i, j: [spot(0, 0, bands)(i, j, 1.0), spot(0, bands, 0)(j, i, -1.0)],
    )
    base += gram_rows(bands, False)
    entries += complex_entries(
        source, base, own, lambda i, j: mirrored(i, j, spot(0, bands, bands))
    )
    base += gram_rows(bands, True)
    entries += complex_entries(
        source, base, every,
        lambda i, j: [spot(1, bands, 0)(i, j, 1.0), spot(1, 0, bands)(j, i, -1.0)],
    )
    source, known, entries = 0, entries, []
    for shift in range(bands // 2 + 1):
        for lane in range(width):
            i = lane // (width // bands)
            j = (i - shift) % bands
            places = [(i, j, 1.0)]
            if shift and 2 * shift != bands:
                places.append((j, i, -1.0))
            for row, column, sign in places:
                real_row, imag_row, at, sign = spot(1, bands, bands)(row, column, sign)
                entries.append((source + 2 * shift, lane, real_row, at, 1.0))
                if shift:
                    entries.append((source + 2 * shift + 1, lane, imag_row, at, sign))
    return known, entries


def solve(system, size, width):
    row_at = lax.broadcasted_iota(jnp.int32, system.shape, 0)
    for k in range(size):
        pivot = system[k : k + 1, :] / system[k : k + 1, k : k + 1]
        system = jnp.where(row_at == k, pivot, system - system[:, k : k + 1] * pivot)
    return system


def wave(length, weight, fraction, indices):
    signed = jnp.where(indices >= length // 2, indices - length, indices).astype(jnp.float32)
    return 2.0 * math.pi / length * (signed + weight * fraction)


class Place:
    def __init__(self, groups, slabs):
        self.groups, self.slabs = groups, slabs
        self.group = lax.axis_index("band")
        self.slab = lax.axis_index("slab")
        self.layer, self.core = self.slab // 2, self.slab % 2
        self.cell = 2 * self.group + self.core

    def slab_peer(self, step):
        slab = lax.rem(self.slab + step, self.slabs)
        return slab, (self.group, slab)

    def band_peer(self, step):
        group = lax.rem(self.group + step, self.groups)
        return group, (group, self.slab)

    def plane_peer(self, step):
        cell = lax.rem(self.cell + step, 2 * self.groups)
        return cell, (cell // 2, 2 * self.layer + cell % 2)


def enter(devices):
    barrier = pltpu.get_barrier_semaphore()
    for device in devices:
        pl.semaphore_signal(barrier, inc=1, device_id=device, device_id_type=MESH)
    pl.semaphore_wait(barrier, len(devices))


def send(source, target, send_sem, recv_sem, device):
    pltpu.make_async_remote_copy(
        src_ref=source,
        dst_ref=target,
        send_sem=send_sem,
        recv_sem=recv_sem,
        device_id=device,
        device_id_type=MESH,
    ).start()


def await_bytes(ref, sem):
    pltpu.make_async_copy(ref, ref, sem).wait()


def total_start(place, mine, first, sems, values):
    mine[0] = values
    first[place.slab] = values
    for step in range(1, place.slabs):
        _, device = place.slab_peer(step)
        send(mine.at[0], first.at[place.slab], sems.at[0], sems.at[1], device)


def total_turn(place, mine, first, second, sems):
    await_bytes(first.at[pl.ds(0, place.slabs - 1)], sems.at[1])
    values = first[0]
    for slab in range(1, place.slabs):
        values = values + first[slab]
    mine[1] = values
    second[place.group] = values
    for step in range(1, place.groups):
        _, device = place.band_peer(step)
        send(mine.at[1], second.at[place.group], sems.at[2], sems.at[3], device)


def total_end(place, first, second, sems):
    await_bytes(second.at[pl.ds(0, place.groups - 1)], sems.at[3])
    values = second[0]
    for group in range(1, place.groups):
        values = values + second[group]
    await_bytes(first.at[pl.ds(0, place.slabs - 1)], sems.at[0])
    await_bytes(second.at[pl.ds(0, place.groups - 1)], sems.at[2])
    return values


def lane_sums(tile, acc):
    rows = acc.shape[0]
    tile[...] = jnp.zeros_like(tile)
    tile[:rows, :] = jnp.sum(acc[...], axis=1)
    ones = jnp.ones((8, tile.shape[1]), jnp.float32)
    return lax.dot_general(
        ones, tile[...], (((1,), (1,)), ((), ())), precision=HIGHEST,
        preferred_element_type=jnp.float32,
    )


def step_kernel(
    groups, slabs, arrays, all_sources,
    permittivity, bloch, given, *refs,
):
    outside, refs = (given, *refs[: arrays - 1]), refs[arrays - 1 :]
    (search, results), inside, refs = refs[:2], refs[2 : arrays + 2], refs[arrays + 2 :]
    block, materials, x_split, x_minus, y_plus, y_minus = inside[:6]
    z_plus, z_minus = inside[6:8] if arrays == 16 else (y_plus, y_minus)
    (
        solve_spread, solve_gather, side_spread, side_gather,
        known_spread, known_gather, field_spread, field_gather,
    ) = inside[-8:]
    solve_sources, side_sources, known_sources, field_sources = all_sources
    (
        work, image, out_y, in_z, out_z, in_y, out_x, eta, local_eta, cells, waves, depths, mixing,
        own_acc, cross_acc, first_tile, own_mine, own_slab, own_band,
        cross_mine, cross_slab, cross_band,
        second_acc, field_acc, second_tile, second_mine, second_slab, second_band,
        field_mine, field_slab, field_band, inverse,
        sems, comes, ends, tail, paths, loads,
    ) = refs
    place = Place(groups, slabs)
    bands, _, _, depth, rows, width = block.shape
    half = depth // 2
    height = rows * slabs
    length = depth * groups
    share = out_y.shape[3] // half
    cell_count = length * height * width
    thin = length // slabs
    chunks = half
    parts = share // 8
    lead = min(WINDOW, chunks)

    for place_of, (source, target) in enumerate(zip(outside, inside)):
        pltpu.make_async_copy(source, target, loads.at[place_of]).start()

    enter(
        [place.slab_peer(i)[1] for i in range(1, slabs)]
        + [
            (lax.rem(place.group + i, groups), 2 * place.layer + core)
            for i in range(1, groups)
            for core in range(2)
        ]
    )

    def send_out(k):
        for i in range(1, slabs):
            slab, device = place.slab_peer(i)
            send(
                given.at[slab // 2, :, :, pl.ds(half * (slab % 2) + k, 1), :, :],
                work.at[:, :, pl.ds(k, 1), pl.ds(rows * place.slab, rows), :],
                sems.at[0, k], sems.at[1, k], device,
            )

    @pl.loop(0, lead)
    def _(k):
        send_out(k)

    for place_of, (source, target) in enumerate(zip(outside, inside)):
        pltpu.make_async_copy(source, target, loads.at[place_of]).wait()

    @pl.loop(0, thin)
    def _(z):
        for cell in range(2 * groups):
            for part in range(parts):
                found = materials[z, pl.ds(cell * share + part * 8, 8), :]
                values = jnp.zeros(found.shape, jnp.float32)
                for material in range(permittivity.shape[0]):
                    values = jnp.where(found == material, permittivity[material] / cell_count, values)
                cells[cell, pl.ds((part * thin + z) * 8, 8), :] = values

    reach = slabs // 4
    first_layer = reach * (place.layer // reach)
    mirror = slabs // 2 - 1 - place.layer

    def near_peer(step):
        layer = first_layer + lax.rem(place.layer - first_layer + step, reach)
        return layer

    def cell_rows(part, slab):
        return pl.ds((part * length + thin * slab) * 8, thin * 8)

    def send_cells(part, layer, core, send_sem, recv_sem):
        send(
            cells.at[2 * place.group + core, pl.ds(part * thin * 8, thin * 8), :],
            eta.at[cell_rows(part, place.slab), :],
            send_sem, recv_sem, (place.group, 2 * layer + core),
        )

    def send_near(part):
        for i in range(1, reach):
            for core in range(2):
                send_cells(part, near_peer(i), core, paths.at[0, part], paths.at[1, part])
        send_cells(part, place.layer, 1 - place.core, paths.at[0, part], paths.at[1, part])

    def hand_on(part):
        await_bytes(eta.at[pl.ds(0, 2 * thin * 8), :], paths.at[3, part])
        for i in range(1, reach):
            for core in range(2):
                at = cell_rows(part, 2 * mirror + core)
                send(
                    eta.at[at, :], eta.at[at, :], paths.at[4, part], paths.at[5, part],
                    (place.group, 2 * near_peer(i) + place.core),
                )

    for part in range(parts):
        target = pl.ds((part * length + thin * place.slab) * 8, thin * 8)
        eta[target, :] = cells[place.cell, pl.ds(part * thin * 8, thin * 8), :]

    fraction = (bloch[0].astype(jnp.float32) + 1.0) / KPOINTS
    at_x = lax.broadcasted_iota(jnp.int32, (height, width), 1)
    at_y = lax.broadcasted_iota(jnp.int32, (height, width), 0)
    wave_x, wave_y = wave(width, 0.5, fraction, at_x), wave(height, 0.35, fraction, at_y)
    planar = jnp.sqrt(wave_x * wave_x + wave_y * wave_y)
    waves[0], waves[1], waves[2] = wave_x / planar, wave_y / planar, planar

    @pl.loop(0, depth)
    def _(z):
        at_z = jnp.broadcast_to(place.group * depth + z, (8, width))
        depths[z] = wave(length, 0.2, fraction, at_z)

    own_acc[...] = jnp.zeros_like(own_acc)
    cross_acc[...] = jnp.zeros_like(cross_acc)
    gram(own_acc, 0, True, block, block, depth, lambda t: t)
    total_start(place, own_mine, own_slab, tail.at[0], lane_sums(first_tile, own_acc))

    @pl.loop(0, chunks)
    def _(z):
        await_bytes(
            work.at[:, :, pl.ds(0, 1), pl.ds(0, rows * (slabs - 1)), :], sems.at[1, z]
        )

        @pl.when(z + lead < chunks)
        def _():
            send_out(z + lead)

        for part in range(parts):

            @pl.when(z == 1 + 4 * part)
            def _(part=part):
                send_near(part)

        for part in range(parts):

            @pl.when(z == chunks - parts + part)
            def _(part=part):
                for core in range(2):
                    send_cells(part, mirror, core, paths.at[2, part], paths.at[3, part])

        for comp in range(2):
            for ri in range(2):
                work[comp, ri, z, pl.ds(rows * place.slab, rows), :] = block[
                    place.layer, comp, ri, half * place.core + z
                ]
        across, along, planar = waves[0], waves[1], waves[2]
        deep = depths[half * place.core + z, 0:1, :]
        size = jnp.sqrt(planar * planar + deep * deep)
        fields = []
        for ri in range(2):
            one = work[0, ri, z]
            two = work[1, ri, z] * size
            upright = one * deep
            fields.append(
                [across * upright - along * two, along * upright + across * two, -planar * one]
            )
        curled = jnp.concatenate(
            [jnp.concatenate([fields[0][c], fields[1][c]], 1) for c in range(3)], 0
        )
        lines = right_transform(curled, x_split.at[0])
        stacked = jnp.concatenate(
            [
                jnp.concatenate(
                    [
                        lines[c * height : (c + 1) * height, :width],
                        lines[c * height : (c + 1) * height, width:],
                    ],
                    0,
                )
                for c in range(3)
            ],
            1,
        )
        planes = left_transform(y_plus, stacked)
        for c in range(3):
            for ri in range(2):
                for cell in range(2 * groups):
                    for part in range(parts):
                        base = ri * height + cell * share + part * 8
                        out_y[cell, c, ri, pl.ds((part * half + z) * 8, 8), :] = planes[
                            base : base + 8, c * width : (c + 1) * width
                        ]

        for part in range(parts):
            source = pl.ds((part * half + z) * 8, 8)
            target = pl.ds((part * length + place.cell * half + z) * 8, 8)
            for i in range(1, 2 * groups):
                cell, device = place.plane_peer(i)
                send(
                    out_y.at[cell, :, :, source, :],
                    in_z.at[:, :, target, :],
                    sems.at[2, z], comes.at[part, z], device,
                )
            for c in range(3):
                for ri in range(2):
                    in_z[c, ri, target, :] = out_y[place.cell, c, ri, source, :]

    def columns_of(source, c, first):
        return jnp.concatenate(
            [
                jnp.concatenate(
                    [source[c, ri, pl.ds(first + j, length, stride=8), :] for ri in range(2)], 0
                )
                for j in range(2)
            ],
            1,
        )

    def keep_columns(target, c, first, values):
        for j in range(2):
            for ri in range(2):
                target[c, ri, pl.ds(first + j, length, stride=8), :] = values[
                    ri * length : (ri + 1) * length, j * width : (j + 1) * width
                ]

    hand_on(0)
    for part in range(parts):
        @pl.loop(0, chunks)
        def _(k, part=part):
            await_bytes(in_z.at[:, :, pl.ds(0, 8 * (2 * groups - 1)), :], comes.at[part, k])

        @pl.loop(0, 4)
        def _(pair, part=part):
            first = part * length * 8 + 2 * pair
            for c in range(3):
                keep_columns(in_z, c, first, left_transform(z_plus, columns_of(in_z, c, first)))

    for part in range(1, parts):
        hand_on(part)
    total_turn(place, own_mine, own_slab, own_band, tail.at[0])

    def send_back(k, part):
        for i in range(1, 2 * groups):
            cell, device = place.plane_peer(i)
            send(
                out_z.at[:, :, pl.ds((part * length + cell * half + k) * 8, 8), :],
                in_y.at[place.cell, :, :, pl.ds((part * half + k) * 8, 8), :],
                sems.at[4, k], sems.at[5, k], device,
            )

    for part in range(parts):
        await_bytes(eta.at[pl.ds(0, thin * 8 * (2 * reach - 1)), :], paths.at[1, part])
        if reach > 1:
            await_bytes(eta.at[pl.ds(0, thin * 16 * (reach - 1)), :], paths.at[5, part])

        @pl.loop(0, 4)
        def _(pair, part=part):
            first = part * length * 8 + 2 * pair
            weight = jnp.concatenate(
                [eta[pl.ds(first + j, length, stride=8), :] for j in range(2)], 1
            )
            weight = jnp.concatenate([weight, weight], 0)
            for c in range(3):
                field = columns_of(in_z, c, first) * weight
                keep_columns(out_z, c, first, left_transform(z_minus, field))

        send_back(0, part)

    @pl.loop(1, lead)
    def _(k):
        for part in range(parts):
            send_back(k, part)

    @pl.loop(0, chunks)
    def _(z):
        for c in range(3):
            for ri in range(2):
                for part in range(parts):
                    in_y[place.cell, c, ri, pl.ds((part * half + z) * 8, 8), :] = out_z[
                        c, ri, pl.ds((part * length + place.cell * half + z) * 8, 8), :
                    ]
        await_bytes(in_y.at[pl.ds(0, 2 * groups - 1), :, :, pl.ds(0, share), :], sems.at[5, z])

        @pl.when(z + lead < chunks)
        def _():
            for part in range(parts):
                send_back(z + lead, part)


        stacked = jnp.concatenate(
            [
                jnp.concatenate(
                    [
                        in_y[cell, c, ri, pl.ds((part * half + z) * 8, 8), :]
                        for ri in range(2)
                        for cell in range(2 * groups)
                        for part in range(parts)
                    ],
                    0,
                )
                for c in range(3)
            ],
            1,
        )
        planes = left_transform(y_minus, stacked)
        lines = jnp.concatenate(
            [
                jnp.concatenate(
                    [
                        planes[:height, c * width : (c + 1) * width],
                        planes[height:, c * width : (c + 1) * width],
                    ],
                    1,
                )
                for c in range(3)
            ],
            0,
        )
        curled = right_transform(lines, x_minus)
        across, along, planar = waves[0], waves[1], waves[2]
        deep = depths[half * place.core + z, 0:1, :]
        size = jnp.sqrt(planar * planar + deep * deep)
        for ri in range(2):
            fields = [
                curled[c * height : (c + 1) * height, ri * width : (ri + 1) * width]
                for c in range(3)
            ]
            work[0, ri, z] = deep * (across * fields[0] + along * fields[1]) - planar * fields[2]
            work[1, ri, z] = size * (across * fields[1] - along * fields[0])
        for comp in range(2):
            for ri in range(2):
                image[place.layer, comp, ri, half * place.core + z] = work[
                    comp, ri, z, pl.ds(rows * place.slab, rows), :
                ]

        for i in range(1, slabs):
            slab, device = place.slab_peer(i)
            send(
                work.at[:, :, pl.ds(z, 1), pl.ds(rows * slab, rows), :],
                image.at[place.layer, :, :, pl.ds(half * place.core + z, 1), :, :],
                sems.at[6, z], sems.at[7, z], device,
            )

    own_sums = total_end(place, own_slab, own_band, tail.at[0])
    pieces = lambda values, row: [
        values[row : row + 1, at : at + width] for at in range(0, values.shape[1], width)
    ]
    system = scatter(pieces(own_sums, 0), solve_sources, solve_spread, solve_gather)
    rows_at = lax.broadcasted_iota(jnp.int32, system.shape, 0)
    lanes_at = lax.broadcasted_iota(jnp.int32, system.shape, 1)
    inverse[...] = solve(
        jnp.where(lanes_at == rows_at + 2 * bands, 1.0, system), 2 * bands, width
    )

    @pl.loop(0, chunks)
    def _(k):
        await_bytes(
            work.at[:, :, pl.ds(0, 1), pl.ds(0, rows * (slabs - 1)), :], sems.at[7, k]
        )
        gram(
            cross_acc, 0, True, block, image, 2, lambda t: half * t + k,
        )

    total_start(place, cross_mine, cross_slab, tail.at[1], lane_sums(first_tile, cross_acc))
    total_turn(place, cross_mine, cross_slab, cross_band, tail.at[1])
    cross_sums = total_end(place, cross_slab, cross_band, tail.at[1])
    side = scatter(pieces(cross_sums, 0), side_sources, side_spread, side_gather)
    factors = inverse[...]
    system = factors[:, 2 * bands : 2 * bands + 1] * side[0:1, :]
    for k in range(1, 2 * bands):
        system += factors[:, 2 * bands + k : 2 * bands + k + 1] * side[k : k + 1, :]
    for row in range(2 * bands):
        for j in range(bands):
            mixing[row, j] = jnp.broadcast_to(
                system[row : row + 1, j : j + 1], (8, width)
            )

    @pl.loop(0, chunks)
    def _(k):
        slab_bytes = work.at[:, :, pl.ds(0, 1), pl.ds(0, rows * (slabs - 1)), :]
        plane_bytes = in_z.at[:, :, pl.ds(0, share * (2 * groups - 1)), :]
        await_bytes(slab_bytes, sems.at[0, k])
        await_bytes(plane_bytes, sems.at[2, k])
        await_bytes(plane_bytes, sems.at[4, k])
        await_bytes(slab_bytes, sems.at[6, k])

    for part in range(parts):
        await_bytes(eta.at[pl.ds(0, thin * 8 * (2 * reach - 1)), :], paths.at[0, part])
        await_bytes(eta.at[pl.ds(0, thin * 16), :], paths.at[2, part])
        if reach > 1:
            await_bytes(eta.at[pl.ds(0, thin * 16 * (reach - 1)), :], paths.at[4, part])

    quarter = width // groups
    second_acc[...] = jnp.zeros_like(second_acc)
    field_acc[...] = jnp.zeros_like(field_acc)
    lane = lax.broadcasted_iota(jnp.int32, (1, width), 1) // quarter
    deep_step = 8 if depth % 8 == 0 else 1

    def send_rows(k, first, count):
        part, c = k // 3, k % 3
        base = (part * length + depth * place.group) * 8
        for i in range(1, groups):
            group, device = place.band_peer(i)
            send(
                out_x.at[part * groups + group, c, :, pl.ds(first, count), :],
                in_z.at[c, :, pl.ds(base + first, count), :],
                ends.at[0, k], ends.at[1, k], device,
            )

    def send_quarter(k):
        send_rows(k, 0, depth * 8)

    @pl.loop(0, parts)
    def _(part):
        band_rows = pl.ds(part * 8, 8)
        across, along, planar = (
            waves[i, pl.ds(rows * place.slab + part * 8, 8), :] for i in range(3)
        )

        @pl.loop(0, depth // deep_step)
        def _(group):
            @pl.loop(group * deep_step, (group + 1) * deep_step)
            def _(z):
                tile_at = (z, band_rows, slice(None))
                deep = depths[z]
                scale = 1.0 / (planar * planar + deep * deep + 1.0)
                for comp in range(2):
                    reals = [block[(i, comp, 0) + tile_at] for i in range(bands)]
                    imags = [block[(i, comp, 1) + tile_at] for i in range(bands)]
                    for j in range(bands):
                        real = image[(j, comp, 0) + tile_at]
                        imag = image[(j, comp, 1) + tile_at]
                        for i in range(bands):
                            real = real - (reals[i] * mixing[i, j] - imags[i] * mixing[bands + i, j])
                            imag = imag - (reals[i] * mixing[bands + i, j] + imags[i] * mixing[i, j])
                        search[(j, comp, 0) + tile_at] = real * scale
                        search[(j, comp, 1) + tile_at] = imag * scale

            planes = pl.ds(group * deep_step, deep_step)
            deep = depths[planes]
            size = jnp.sqrt(planar * planar + deep * deep)
            count = deep_step * 8
            lines = []
            for i in range(bands):
                fields = []
                for ri in range(2):
                    one = search[i, 0, ri, planes, band_rows, :]
                    two = search[i, 1, ri, planes, band_rows, :] * size
                    upright = one * deep
                    fields.append(
                        [
                            value.reshape(count, width)
                            for value in (
                                across * upright - along * two,
                                along * upright + across * two,
                                -planar * one,
                            )
                        ]
                    )
                curled = jnp.concatenate(
                    [jnp.concatenate([fields[0][c], fields[1][c]], 1) for c in range(3)], 0
                )
                lines.append(right_transform(curled, x_split.at[i]))
            at = pl.ds(group * count, count)
            for target in range(groups):
                for ri in range(2):
                    columns = slice(ri * width, (ri + 1) * width)
                    packed = lines[(-target) % groups][:, columns]
                    for spot in range(1, groups):
                        packed = jnp.where(
                            lane == spot, lines[(spot - target) % groups][:, columns], packed
                        )
                    for c in range(3):
                        out_x[part * groups + target, c, ri, at, :] = packed[c * count : (c + 1) * count]

            @pl.when(part == 0)
            def _():
                send_rows(0, group * count, count)

        for c in range(3):
            for ri in range(2):
                in_z[c, ri, pl.ds((part * length + depth * place.group) * 8, depth * 8), :] = out_x[
                    part * groups + place.group, c, ri
                ]

    @pl.loop(0, 3 * parts)
    def _(k):
        part, c = k // 3, k % 3
        await_bytes(in_z.at[c, :, pl.ds(0, depth * 8 * (groups - 1)), :], ends.at[1, k])

        @pl.when(k == 0)
        def _():
            send_quarter(1)

        @pl.when(k + 2 < 3 * parts)
        def _():
            send_quarter(k + 2)

        base = part * length * 8

        @pl.loop(0, 4)
        def _(pair):
            first = base + 2 * pair
            keep_columns(out_z, c, first, left_transform(z_plus, columns_of(in_z, c, first)))

        for i in range(1, slabs):
            slab, device = place.slab_peer(i)
            send(
                out_z.at[c, :, pl.ds(base + thin * 8 * slab, thin * 8), :],
                in_y.at[place.slab, c, :, pl.ds(part * thin * 8, thin * 8), :],
                ends.at[2, k], ends.at[3, k], device,
            )
        for ri in range(2):
            in_y[place.slab, c, ri, pl.ds(part * thin * 8, thin * 8), :] = out_z[
                c, ri, pl.ds(base + thin * 8 * place.slab, thin * 8), :
            ]

    @pl.loop(0, thin)
    def _(z):
        for cell in range(2 * groups):
            for part in range(parts):
                values = cells[cell, pl.ds((part * thin + z) * 8, 8), :]
                values = pltpu.roll(values, lax.rem(width - quarter * place.group, width), 1)
                values = jnp.where(lane == 0, values, 0.0)
                reach = quarter
                while reach < width:
                    values = values + pltpu.roll(values, reach, 1)
                    reach *= 2
                local_eta[z, cell * share + part * 8 : cell * share + part * 8 + 8, :] = values

    base = gram(second_acc, 0, False, block, search, depth, lambda t: t)
    base = gram(second_acc, base, True, search, search, depth, lambda t: t)
    gram(second_acc, base, False, search, image, depth, lambda t: t)
    total_start(place, second_mine, second_slab, tail.at[2], lane_sums(second_tile, second_acc))

    def add_products(real, imag, weight):
        real_weighted, imag_weighted = real * weight, imag * weight
        for shift in range(bands // 2 + 1):
            if shift == 0:
                real_other, imag_other = real, imag
            else:
                real_other = pltpu.roll(real, quarter * shift, 1)
                imag_other = pltpu.roll(imag, quarter * shift, 1)
            real_term = real_weighted * real_other + imag_weighted * imag_other
            imag_term = real_weighted * imag_other - imag_weighted * real_other
            for place_of, term in ((2 * shift, real_term), (2 * shift + 1, imag_term)):
                field_acc[place_of] += jnp.sum(term.reshape(height // 8, 8, width), axis=0)

    for c in range(3):
        for part in range(parts):
            await_bytes(
                in_y.at[pl.ds(0, slabs - 1), c, :, pl.ds(0, thin * 8), :],
                ends.at[3, part * 3 + c],
            )

        @pl.loop(0, thin // 2)
        def _(pair, c=c):
            stacked = jnp.concatenate(
                [
                    jnp.concatenate(
                        [
                            in_y[slab, c, ri, pl.ds(part * thin * 8 + 16 * pair + 8 * j, 8), :]
                            for ri in range(2)
                            for slab in range(slabs)
                            for part in range(parts)
                        ],
                        0,
                    )
                    for j in range(2)
                ],
                1,
            )
            planes = left_transform(y_plus, stacked)
            for j in range(2):
                lanes = slice(j * width, (j + 1) * width)
                add_products(planes[:height, lanes], planes[height:, lanes], local_eta[2 * pair + j])

    fields = jnp.sum(field_acc[...], axis=1)
    fields = pltpu.roll(fields, lax.rem(width - quarter * place.group, width), 1)
    total_start(place, field_mine, field_slab, tail.at[3], fields)
    total_turn(place, second_mine, second_slab, second_band, tail.at[2])
    total_turn(place, field_mine, field_slab, field_band, tail.at[3])
    second_sums = total_end(place, second_slab, second_band, tail.at[2])
    listed = pieces(own_sums, 0) + pieces(cross_sums, 0) + pieces(second_sums, 0)
    known = scatter(listed, known_sources, known_spread, known_gather)
    fields = total_end(place, field_slab, field_band, tail.at[3])
    listed = [fields[row : row + 1] for row in range(2 * (bands // 2 + 1))]
    fields = scatter(listed, field_sources, field_spread, field_gather)
    results[...] = (known + fields) / cell_count

    @pl.loop(0, 3 * parts)
    def _(k):
        await_bytes(in_z.at[0, :, pl.ds(0, depth * 8 * (groups - 1)), :], ends.at[0, k])
        await_bytes(in_y.at[pl.ds(0, slabs - 1), 0, :, pl.ds(0, thin * 8), :], ends.at[2, k])


def vmem(count):
    return [pl.BlockSpec(memory_space=pltpu.VMEM)] * count


def round_up(value, step):
    return -(-value // step) * step


def step(block, materials, permittivity, bloch, groups, slabs):
    bands, _, _, depth, rows, width = block.shape
    half, height, length = depth // 2, rows * slabs, depth * groups
    share = height // (2 * groups)
    thin, parts, quarter = length // slabs, rows // 8, width // groups
    chunks = half
    first_count = gram_rows(bands, True)
    first_lanes = round_up(first_count, width)
    second_count = 2 * gram_rows(bands, False) + gram_rows(bands, True)
    second_lanes = round_up(second_count, width)
    field_rows = round_up(2 * (bands // 2 + 1), 8)

    plain = dft_matrix(width, 1.0).T
    orders = []
    for band in range(bands):
        spots = np.arange(width) // quarter
        source = ((spots - band) % groups) * quarter + np.arange(width) % quarter
        orders.append(right_table(plain[:, np.concatenate([source, width + source])]))
    first_pieces, second_pieces = first_lanes // width, second_lanes // width
    known, fields = result_entries(bands, width, first_pieces, second_pieces)
    scattered = [
        scatter_tables(entries, count, width)
        for entries, count in (
            (system_entries(bands), first_pieces),
            (side_entries(bands), first_pieces),
            (known, 2 * first_pieces + second_pieces),
            (fields, 2 * (bands // 2 + 1)),
        )
    ]
    tables = [
        np.stack(orders),
        right_table(dft_matrix(width, -1.0).T),
        left_table(height, 1.0),
        left_table(height, -1.0),
        *([] if length == height else [left_table(length, 1.0), left_table(length, -1.0)]),
        *[table for _, *pair in scattered for table in pair],
    ]
    single = lambda *shape: pltpu.VMEM(shape, jnp.float32)
    slots = lambda *tile: [single(2, *tile), single(slabs, *tile), single(groups, *tile)]
    by_cell = (2 * groups, 3, 2, half * share, width)
    by_part = (parts * groups, 3, 2, depth * 8, width)
    out_x = [] if by_cell == by_part else [single(*by_part)]
    kernel = partial(
        step_kernel, groups, slabs, 2 + len(tables), [sources for sources, *_ in scattered]
    )

    def body(*refs):
        refs = list(refs)
        if not out_x:
            outgoing = 2 + 2 * (2 + len(tables)) + 2 + 2
            refs.insert(outgoing + 4, refs[outgoing])
        kernel(*refs)

    return pl.pallas_call(
        body,
        in_specs=[pl.BlockSpec(memory_space=pltpu.SMEM)] * 2 + [pl.BlockSpec(memory_space=pl.ANY)] * (2 + len(tables)),
        out_specs=vmem(2),
        out_shape=[
            pltpu.VMEM(block.shape, jnp.float32),
            jax.ShapeDtypeStruct((8 * bands, width), jnp.float32),
        ],
        scratch_shapes=[
            *[pltpu.VMEM(array.shape, array.dtype) for array in (block, materials, *tables)],
            single(2, 2, half, height, width),
            single(*block.shape),
            single(*by_cell),
            single(3, 2, length * share, width),
            single(3, 2, length * share, width),
            single(*by_cell),
            *out_x,
            single(length * share, width),
            single(thin, height, width),
            single(2 * groups, thin * share, width),
            single(3, height, width),
            single(depth, 8, width),
            single(2 * bands, bands, 8, width),
            single(first_count, 8, width),
            single(first_count, 8, width),
            single(first_lanes, width),
            *slots(8, first_lanes),
            *slots(8, first_lanes),
            single(second_count, 8, width),
            single(field_rows, 8, width),
            single(second_lanes, width),
            *slots(8, second_lanes),
            *slots(field_rows, width),
            single(2 * bands, width),
            pltpu.SemaphoreType.DMA((8, chunks)),
            pltpu.SemaphoreType.DMA((parts, chunks)),
            pltpu.SemaphoreType.DMA((4, 3 * parts)),
            pltpu.SemaphoreType.DMA((4, 4)),
            pltpu.SemaphoreType.DMA((6, parts)),
            pltpu.SemaphoreType.DMA((2 + len(tables),)),
        ],
        compiler_params=pltpu.CompilerParams(
            collective_id=0, has_side_effects=True, vmem_limit_bytes=VMEM_LIMIT
        ),
    )(permittivity, bloch, block, materials, *[jnp.asarray(table) for table in tables])


def shards(band_block, material_grid, inverse_permittivity, bloch_index):
    groups, slabs = lax.axis_size("band"), lax.axis_size("slab")
    size = 2 * band_block.shape[0]
    search_block, results = step(
        band_block, material_grid, inverse_permittivity, bloch_index, groups, slabs
    )
    results = results[:, :size].reshape(2, 2, size, size)
    return (search_block, results[0], results[1])


def solution(mesh):
    return jax.shard_map(
        shards,
        mesh=mesh,
        in_specs=(P(None, None, None, "band", "slab", None), P("slab", None, None), P(), P()),
        out_specs=(P(None, None, None, "band", "slab", None), P(), P()),
        check_vma=False,
    )
```
